256 devices in a mesh: band: 16 (over z_hi, x), plane: 16 (over y, z_lo, core).
Axes of the slice: x: 4, y: 4, z: 8 (z_hi: 4, z_lo: 2; z = z_hi * 2 + z_lo), core: 2. Of those that a mesh axis runs over, the one named last changes fastest.
Arguments:
- orbitals: float32 [16, 112, 12544], P('band', 'plane'), may hold values from -6 to 6
Outputs:
- exchange_w: float32 [16, 112, 12544], P('band', 'plane')
The draws below stay inside these ranges and needn't reach their ends.
All inputs are finite; a program needn't handle non-finite values.
Results may differ from the reference program's by a relative error of at most 0.000082.
Values sent between devices are 32-bit elements; how exact they have to be, the bound alone decides.
A program may use at most 64 MiB of HBM per device.

```python
import math
import jax
import jax.numpy as jnp
from jax import lax

NG = 112
B = 1
ROUNDS = 2
ORB = 16


def block_levels(own_key, shape, pieces, least, largest):
    factor_of = 1.0
    for dim, blocks in pieces:
        steps = jax.random.uniform(jax.random.fold_in(jax.random.fold_in(own_key, 6), dim), (blocks,), jnp.float32, least / len(pieces), largest / len(pieces))
        factor_of = factor_of * jnp.repeat(jnp.exp(steps), shape[dim] // blocks).reshape((-1,) + (1,) * (len(shape) - 1 - dim))
    return factor_of


def noise(rng, dims, width, most, split=(), kind=jnp.bfloat16):
    gain = block_levels(rng, dims, split, -0.22, 0.18) if split else 1.0
    drawn = jax.random.normal(rng, dims, jnp.float32) * width * gain
    return jnp.minimum(jnp.maximum(drawn, -most), most).astype(kind)


def setup_inputs(seed: int = 0) -> dict:
    seeds = jax.random.split(jax.random.key(seed), 2)
    orbitals = noise(seeds[0], (ORB, NG, NG * NG), 1.0, 6.0, ((0, 16), (1, 16)), jnp.float32)
    return dict(orbitals=orbitals)


screen_omega = 0.106
cell_length = 46.93
mixing = 0.25


def wave_number(index, count):
    return jnp.where(2 * index < count, index, index - count)


def kernel_values(squares):
    gsquare = squares * (2.0 * math.pi / cell_length) ** 2
    safe = jnp.where(gsquare > 0, gsquare, 1.0)
    values = 4.0 * math.pi / safe * (1.0 - jnp.exp(-safe / (4.0 * screen_omega * screen_omega)))
    return jnp.where(gsquare > 0, values, math.pi / (screen_omega * screen_omega))


def reference(orbitals):
    field = orbitals.reshape(ORB, NG, NG, NG)
    sources = field[: ROUNDS * B]
    frequency = wave_number(jnp.arange(NG, dtype=jnp.int32), NG).astype(jnp.float32)
    squares = frequency[:, None, None] ** 2 + frequency[None, :, None] ** 2 + frequency[None, None, :] ** 2
    kernel = kernel_values(squares)

    def single(orbital):
        density = orbital[None] * sources
        spectrum = jnp.fft.fftn(density, axes=(1, 2, 3))
        potential = jnp.real(jnp.fft.ifftn(spectrum * kernel, axes=(1, 2, 3)))
        return -mixing * jnp.sum(sources * potential, axis=0)

    result = lax.map(single, field)
    return result.reshape(ORB, NG, NG * NG)
```

```python
import functools
import math

import jax
import jax.numpy as jnp
import ml_dtypes
import numpy as np
from jax import lax
from jax.experimental import pallas as pl
from jax.experimental.pallas import tpu as pltpu
from jax.sharding import PartitionSpec as P

MESH = pl.DeviceIdType.MESH
NG = 112
FLAT = NG * NG
HALF = FLAT // 2
CHUNKS = ((0, 3200), (3200, 3072))
SHARES = 16
THICK = NG // SHARES
ROWS = 2 * THICK
BLOCK = 112
USED = THICK * ROWS
screen_omega = 0.106
cell_length = 46.93
mixing = 0.25
f32, bf16 = jnp.float32, jnp.bfloat16


def tables():
    index = np.arange(NG)
    angle = (index[:, None] * index[None, :] % NG) * (2.0 * math.pi / NG)
    cos, sin = np.cos(angle), np.sin(angle)
    re, im = slice(0, NG), slice(128, 128 + NG)
    last = np.zeros((256, 256))
    last[re, re], last[im, re] = cos, sin
    last[re, im], last[im, im] = -sin, cos
    last_back = np.zeros((256, 256))
    last_back[re, re], last_back[im, re] = cos, -sin
    last_back[re, im], last_back[im, im] = sin, cos
    second = np.zeros((256, 256))
    second_back = np.zeros((256, 256))
    for share in range(SHARES):
        for part in range(2):
            for k in range(THICK):
                row, wave = 16 * share + THICK * part + k, THICK * share + k
                if part == 0:
                    second[row, 0:NG], second[row, NG : 2 * NG] = cos[wave], sin[wave]
                    second_back[0:NG, row], second_back[NG : 2 * NG, row] = cos[wave], sin[wave]
                else:
                    second[row, 0:NG], second[row, NG : 2 * NG] = -sin[wave], cos[wave]
                    second_back[0:NG, row], second_back[NG : 2 * NG, row] = -sin[wave], cos[wave]
    place = 8 * (index // THICK) + index % THICK
    first = np.zeros((256, 256))
    first_back = np.zeros((256, 256))
    first[re, place], first[re, 128 + place] = cos, sin
    first[im, place], first[im, 128 + place] = -sin, cos
    first_back[place, re], first_back[place, im] = cos, -sin
    first_back[128 + place, re], first_back[128 + place, im] = sin, cos
    both = []
    for table in (last, second, first, first_back, second_back, last_back):
        high = table.astype(ml_dtypes.bfloat16)
        both += [high, (table - high.astype(np.float64)).astype(ml_dtypes.bfloat16)]
    return np.stack(both)


def split(values):
    high = values.astype(bf16)
    return high, (values - high.astype(f32)).astype(bf16)


def dot(a, b):
    return jnp.dot(a, b, preferred_element_type=f32)


def from_left(high, low, values):
    big, small = split(values)
    return dot(high, big) + dot(high, small) + dot(low, big)


def from_right(values, high, low):
    big, small = split(values)
    return dot(big, high) + dot(small, high) + dot(big, low)


def kernel_tile(k_second, shape):
    def wave(index):
        return jnp.where(2 * index < NG, index, index - NG).astype(f32)

    first = wave(lax.broadcasted_iota(jnp.int32, shape, 0))
    last = wave(lax.broadcasted_iota(jnp.int32, shape, 1))
    second = wave(jnp.full(shape, k_second, jnp.int32))
    gsquare = (first * first + second * second + last * last) * (2.0 * math.pi / cell_length) ** 2
    safe = jnp.where(gsquare > 0, gsquare, 1.0)
    values = 4.0 * math.pi / safe * (1.0 - jnp.exp(-safe / (4.0 * screen_omega * screen_omega)))
    values = jnp.where(gsquare > 0, values, math.pi / (screen_omega * screen_omega))
    return values * (-mixing / float(NG) ** 3)


def body(
    psi_hbm, tab_hbm, out,
    psi, tab, src, work, spec, kern, s_out, r_in, g_out, h_in, sums, srows,
    load_sem, zs, zr, xs, xr, fs, fr, bs, br,
):
    band, me = lax.axis_index("band"), lax.axis_index("plane")
    x, zh = band % 4, band // 4

    def at_x(d):
        return (zh * 4 + (x + d) % 4, me)

    def at_z(d):
        return (((zh + d) % 4) * 4 + x, me)

    def at_plane(d):
        return (band, (me + d) % SHARES)

    barrier = pltpu.get_barrier_semaphore()
    peers = [at_x(d) for d in (1, 2, 3)] + [at_z(1), at_z(3)] + [at_plane(d) for d in range(1, SHARES)]
    for peer in peers:
        pl.semaphore_signal(barrier, inc=1, device_id=peer, device_id_type=MESH)

    load_psi = pltpu.make_async_copy(psi_hbm, psi, load_sem.at[0])
    load_psi.start()
    load_tab = pltpu.make_async_copy(tab_hbm, tab, load_sem.at[1])
    load_tab.start()

    origin = jnp.logical_and(zh == 0, x < 2)

    def piece(which, chunk):
        start, length = CHUNKS[chunk]
        offset = pl.multiple_of((which // 2) * HALF + start, 128)
        return src.at[((which + 1) // 2) % 2, :, pl.ds(offset, length)]

    def own_load(chunk):
        start, length = CHUNKS[chunk]
        return pltpu.make_async_copy(
            psi_hbm.at[:, pl.ds(start, length)], piece(x, chunk), load_sem.at[2 + chunk]
        )

    @pl.when(origin)
    def _():
        for chunk in range(2):
            own_load(chunk).start()

    work[...] = jnp.zeros_like(work)
    for buffer in (s_out, r_in, h_in):
        for share in range(SHARES):
            rows = slice(BLOCK * share + USED, BLOCK * (share + 1))
            buffer[rows, :] = jnp.zeros((BLOCK - USED, 128), f32)
    srows[...] = jnp.zeros_like(srows)
    for k in range(THICK):
        kern[k] = kernel_tile(THICK * me + k, (128, 128))
    load_psi.wait()
    load_tab.wait()

    @pl.when(origin)
    def _():
        for chunk in range(2):
            own_load(chunk).wait()

    pl.semaphore_wait(barrier, len(peers))

    def scatter(chunk):
        start, length = CHUNKS[chunk]
        return pltpu.make_async_remote_copy(
            src_ref=psi.at[:, pl.ds(HALF + start, length)],
            dst_ref=piece(3 - x, chunk),
            send_sem=zs.at[2, chunk], recv_sem=zr.at[chunk],
            device_id=(zh * 4 + 3 - x, me), device_id_type=MESH,
        )

    def up(d, chunk):
        return pltpu.make_async_remote_copy(
            src_ref=piece(x, chunk), dst_ref=piece(x, chunk),
            send_sem=zs.at[0 if d == 1 else 1, chunk], recv_sem=zr.at[chunk],
            device_id=at_z(d), device_id_type=MESH,
        )

    def across(d, chunk):
        return pltpu.make_async_remote_copy(
            src_ref=piece(x, chunk), dst_ref=piece(x, chunk),
            send_sem=xs.at[d - 1, chunk], recv_sem=xr.at[d - 1, chunk],
            device_id=at_x(d), device_id_type=MESH,
        )

    def arrived(chunk):
        up(1, chunk).wait_recv()

    def all_across(chunk):
        for d in (1, 3, 2):
            across(d, chunk).start()

    @pl.when(origin)
    def _():
        for chunk in range(2):
            scatter(chunk).start()

    @pl.when(zh == 0)
    def _():
        for chunk in range(2):
            @pl.when(x >= 2)
            def _():
                arrived(chunk)

            up(1 if chunk == 0 else 3, chunk).start()
            all_across(chunk)
        up(3, 0).start()
        up(1, 1).start()

    @pl.when(zh == 1)
    def _():
        arrived(0)
        up(1, 0).start()
        all_across(0)
        arrived(1)
        all_across(1)

    @pl.when(zh == 3)
    def _():
        arrived(1)
        up(3, 1).start()
        all_across(1)
        arrived(0)
        all_across(0)

    @pl.when(zh == 2)
    def _():
        for chunk in range(2):
            arrived(chunk)
            all_across(chunk)

    for chunk in range(2):
        for d in (1, 2, 3):
            other = (x + 4 - d) % 4
            pltpu.make_async_remote_copy(
                src_ref=piece(x, chunk), dst_ref=piece(other, chunk),
                send_sem=xs.at[d - 1, chunk], recv_sem=xr.at[d - 1, chunk],
                device_id=at_x(d), device_id_type=MESH,
            ).wait_recv()

    field = psi[...]
    for which in range(2):
        density = field * src[which]
        for y in range(NG):
            work[8 * y : 8 * y + THICK, 128 * which : 128 * which + NG] = density[:, NG * y : NG * (y + 1)]
    for part in range(4):
        rows = slice(224 * part, 224 * (part + 1))
        values = from_right(work[rows, :], tab[0], tab[1])
        spec[0, rows, :] = values[:, 0:128]
        spec[1, rows, :] = values[:, 128:256]

    def forward_second(planes):
        columns = []
        for plane in planes:
            columns.append(jnp.concatenate([spec[part, pl.ds(plane, NG, stride=8), :] for part in range(2)], axis=0))
        values = jnp.concatenate(columns, axis=1)
        result = from_left(tab[2, :, 0 : 2 * NG], tab[3, :, 0 : 2 * NG], values)
        for place, plane in enumerate(planes):
            for share in range(SHARES):
                start = BLOCK * share + ROWS * plane
                s_out[start : start + ROWS, :] = result[16 * share : 16 * share + ROWS, 128 * place : 128 * (place + 1)]

    for planes in ((0, 1), (2, 3), (4, 5), (6,)):
        forward_second(planes)

    def block(buffer, share):
        return buffer.at[pl.ds(pl.multiple_of(BLOCK * share, 8), USED)]

    def exchange(source, target, send, receive, d):
        return pltpu.make_async_remote_copy(
            src_ref=block(source, (me + d) % SHARES), dst_ref=block(target, me),
            send_sem=send.at[d - 1], recv_sem=receive.at[d - 1],
            device_id=at_plane(d), device_id_type=MESH,
        )

    def arrival(source, target, send, receive, d):
        return pltpu.make_async_remote_copy(
            src_ref=block(source, me), dst_ref=block(target, (me + SHARES - d) % SHARES),
            send_sem=send.at[d - 1], recv_sem=receive.at[d - 1],
            device_id=at_plane(d), device_id_type=MESH,
        )

    def keep(source, target):
        rows = pl.ds(pl.multiple_of(BLOCK * me, 8), BLOCK)
        target[rows, :] = source[rows, :]

    for d in range(1, SHARES):
        exchange(s_out, r_in, fs, fr, d).start()
    keep(s_out, r_in)
    for which in range(2):
        for y in range(NG):
            srows[which, 8 * y : 8 * y + THICK, 0:NG] = src[which, :, NG * y : NG * (y + 1)]
    for d in range(1, SHARES):
        arrival(s_out, r_in, fs, fr, d).wait_recv()

    def middle(waves):
        columns = []
        for k in waves:
            columns.append(jnp.concatenate(
                [r_in[pl.ds(k, 128, stride=ROWS), :], r_in[pl.ds(THICK + k, 128, stride=ROWS), :]], axis=0))
        spectrum = from_left(tab[4], tab[5], jnp.concatenate(columns, axis=1))
        factor = jnp.concatenate([kern[k] for k in waves], axis=1)
        spectrum = spectrum * jnp.concatenate([factor, factor], axis=0)
        result = from_left(tab[6], tab[7], spectrum)
        for place, k in enumerate(waves):
            lanes = slice(128 * place, 128 * (place + 1))
            g_out[pl.ds(k, 128, stride=ROWS), :] = result[0:128, lanes]
            g_out[pl.ds(THICK + k, 128, stride=ROWS), :] = result[128:256, lanes]

    for waves in ((0, 1), (2, 3), (4, 5), (6,)):
        middle(waves)

    for d in range(1, SHARES):
        exchange(g_out, h_in, bs, br, d).start()
    keep(g_out, h_in)
    for d in range(1, SHARES):
        arrival(g_out, h_in, bs, br, d).wait_recv()

    def back_second(planes):
        columns = []
        for plane in planes:
            columns.append(jnp.concatenate(
                [h_in[BLOCK * q + ROWS * plane : BLOCK * q + ROWS * plane + 16, :] for q in range(SHARES)], axis=0))
        values = from_left(tab[8, 0 : 2 * NG], tab[9, 0 : 2 * NG], jnp.concatenate(columns, axis=1))
        for place, plane in enumerate(planes):
            lanes = slice(128 * place, 128 * (place + 1))
            both = jnp.concatenate([values[0:NG, lanes], values[NG : 2 * NG, lanes]], axis=1)
            potential = from_right(both, tab[10], tab[11])
            rows = pl.ds(plane, NG, stride=8)
            sums[rows, :] = potential[:, 0:128] * srows[0, rows, :] + potential[:, 128:256] * srows[1, rows, :]

    for planes in ((0, 1), (2, 3), (4, 5), (6,)):
        back_second(planes)
    for y in range(NG):
        out[:, NG * y : NG * (y + 1)] = sums[8 * y : 8 * y + THICK, 0:NG]

    @pl.when(origin)
    def _():
        for chunk in range(2):
            scatter(chunk).wait_send()

    @pl.when(zh == 0)
    def _():
        for chunk in range(2):
            up(1, chunk).wait_send()
            up(3, chunk).wait_send()

    @pl.when(zh == 1)
    def _():
        up(1, 0).wait_send()

    @pl.when(zh == 3)
    def _():
        up(3, 1).wait_send()

    for chunk in range(2):
        for d in (1, 2, 3):
            across(d, chunk).wait_send()
    for d in range(1, SHARES):
        exchange(s_out, r_in, fs, fr, d).wait_send()
        exchange(g_out, h_in, bs, br, d).wait_send()


def on_device(orbitals):
    table = jnp.asarray(tables())
    field = orbitals.reshape(THICK, FLAT)
    dma = pltpu.SemaphoreType.DMA
    vmem = pltpu.VMEM
    total = pl.pallas_call(
        body,
        out_shape=jax.ShapeDtypeStruct((THICK, FLAT), f32),
        in_specs=[pl.BlockSpec(memory_space=pl.ANY)] * 2,
        out_specs=pl.BlockSpec(memory_space=vmem),
        scratch_shapes=[
            vmem((THICK, FLAT), f32),
            vmem((12, 256, 256), bf16),
            vmem((2, THICK, FLAT), f32),
            vmem((8 * NG, 256), f32),
            vmem((2, 8 * NG, 128), f32),
            vmem((THICK, 128, 128), f32),
            vmem((SHARES * BLOCK, 128), f32),
            vmem((SHARES * BLOCK, 128), f32),
            vmem((SHARES * BLOCK, 128), f32),
            vmem((SHARES * BLOCK, 128), f32),
            vmem((8 * NG, 128), f32),
            vmem((2, 8 * NG, 128), f32),
            dma((4,)), dma((3, 2)), dma((2,)), dma((3, 2)), dma((3, 2)),
            dma((15,)), dma((15,)), dma((15,)), dma((15,)),
        ],
        compiler_params=pltpu.CompilerParams(collective_id=0, has_side_effects=True),
    )(field, table)
    return total.reshape(orbitals.shape)


def solution(mesh):
    spec = P("band", "plane", None)
    return jax.shard_map(on_device, mesh=mesh, in_specs=(spec,), out_specs=spec, check_vma=False)
```

```python
import math

import jax
import jax.numpy as jnp
import ml_dtypes
import numpy as np
from jax import lax
from jax.experimental import pallas as pl
from jax.experimental.pallas import tpu as pltpu
from jax.sharding import PartitionSpec as P

MESH = pl.DeviceIdType.MESH
NG = 112
FLAT = NG * NG
LINES = FLAT // 128
HALF = LINES // 2
LAG = 3
SHARES = 16
THICK = NG // SHARES
ROWS = 2 * THICK
BLOCK = 112
USED = THICK * ROWS
ORDER = (10, 11, 8, 9, 6, 14, 7, 13, 2, 3, 4, 12, 5, 15, 1)
screen_omega = 0.106
cell_length = 46.93
mixing = 0.25
f32, bf16 = jnp.float32, jnp.bfloat16


def tables():
    index = np.arange(NG)
    angle = (index[:, None] * index[None, :] % NG) * (2.0 * math.pi / NG)
    cos, sin = np.cos(angle), np.sin(angle)
    re, im = slice(0, NG), slice(128, 128 + NG)
    last = np.zeros((256, 256))
    last[re, re], last[im, re] = cos, sin
    last[re, im], last[im, im] = -sin, cos
    last_back = np.zeros((256, 256))
    last_back[re, re], last_back[im, re] = cos, -sin
    last_back[re, im], last_back[im, im] = sin, cos
    second = np.zeros((256, 256))
    second_back = np.zeros((256, 256))
    for share in range(SHARES):
        for part in range(2):
            for k in range(THICK):
                row, wave = 16 * share + THICK * part + k, THICK * share + k
                if part == 0:
                    second[row, 0:NG], second[row, NG : 2 * NG] = cos[wave], sin[wave]
                    second_back[0:NG, row], second_back[NG : 2 * NG, row] = cos[wave], sin[wave]
                else:
                    second[row, 0:NG], second[row, NG : 2 * NG] = -sin[wave], cos[wave]
                    second_back[0:NG, row], second_back[NG : 2 * NG, row] = -sin[wave], cos[wave]
    place = 8 * (index // THICK) + index % THICK
    first = np.zeros((256, 256))
    first_back = np.zeros((256, 256))
    first[re, place], first[re, 128 + place] = cos, sin
    first[im, place], first[im, 128 + place] = -sin, cos
    first_back[place, re], first_back[place, im] = cos, -sin
    first_back[128 + place, re], first_back[128 + place, im] = sin, cos
    both = []
    for table in (last, second, first, first_back, second_back, last_back):
        high = table.astype(ml_dtypes.bfloat16)
        both += [high, (table - high.astype(np.float64)).astype(ml_dtypes.bfloat16)]
    return np.stack(both)


def split(values):
    high = values.astype(bf16)
    return high, (values - high.astype(f32)).astype(bf16)


def dot(a, b):
    return jnp.dot(a, b, preferred_element_type=f32)


def from_left(high, low, values):
    big, small = split(values)
    return dot(high, big) + dot(high, small) + dot(low, big)


def from_right(values, high, low):
    big, small = split(values)
    return dot(big, high) + dot(small, high) + dot(big, low)


def kernel_tile(k_second, shape):
    def wave(index):
        return jnp.where(2 * index < NG, index, index - NG).astype(f32)

    first = wave(lax.broadcasted_iota(jnp.int32, shape, 0))
    last = wave(lax.broadcasted_iota(jnp.int32, shape, 1))
    second = wave(jnp.full(shape, k_second, jnp.int32))
    gsquare = (first * first + second * second + last * last) * (2.0 * math.pi / cell_length) ** 2
    safe = jnp.where(gsquare > 0, gsquare, 1.0)
    values = 4.0 * math.pi / safe * (1.0 - jnp.exp(-safe / (4.0 * screen_omega * screen_omega)))
    values = jnp.where(gsquare > 0, values, math.pi / (screen_omega * screen_omega))
    return values * (-mixing / float(NG) ** 3)


def kernel_axes():
    band = lax.axis_index("band")
    return band % 4, band // 4, lax.axis_index("plane")


def send(source, target, send_sem, recv_sem, device):
    return pltpu.make_async_remote_copy(
        src_ref=source, dst_ref=target, send_sem=send_sem, recv_sem=recv_sem,
        device_id=device, device_id_type=MESH,
    )


def spread(psi_hbm, half_hbm, send_sem, recv_sem):
    x, zh, me = kernel_axes()

    def half(i):
        return send(
            psi_hbm.at[pl.ds(LINES * i + HALF, HALF), 0], half_hbm.at[i, pl.ds(0, HALF)],
            send_sem.at[i], recv_sem.at[i], (zh * 4 + 3 - x, me),
        )

    @pl.when(zh == 0)
    def _():
        barrier = pltpu.get_barrier_semaphore()
        pl.semaphore_signal(barrier, inc=1, device_id=(zh * 4 + 3 - x, me), device_id_type=MESH)
        pl.semaphore_wait(barrier, 1)

        @pl.when(x < 2)
        def _():
            for i in range(THICK):
                half(i).start()
            for i in range(THICK):
                half(i).wait_send()

        @pl.when(x >= 2)
        def _():
            for i in range(THICK):
                half(i).wait_recv()


def body(
    psi_hbm, half_hbm, tab_hbm, out,
    psi, tab, src, psi_y, src_y, kern, s_out, r_in, g_out, h_in,
    load_sem, own_sem, zs, zr, xs, xr, fs, fr, bs, br,
):
    x, zh, me = kernel_axes()
    band = zh * 4 + x

    def at_x(d):
        return (zh * 4 + (x + d) % 4, me)

    def at_z(d):
        return (((zh + d) % 4) * 4 + x, me)

    def at_plane(d):
        return (band, (me + d) % SHARES)

    barrier = pltpu.get_barrier_semaphore()
    peers = [at_x(d) for d in (1, 2, 3)] + [at_z(d) for d in (1, 2, 3)]
    peers += [at_plane(d) for d in range(1, SHARES)]
    for peer in peers:
        pl.semaphore_signal(barrier, inc=1, device_id=peer, device_id_type=MESH)

    load_psi = pltpu.make_async_copy(psi_hbm.at[:, 0], psi, load_sem.at[0])
    load_psi.start()
    load_tab = pltpu.make_async_copy(tab_hbm, tab, load_sem.at[1])
    load_tab.start()

    own_source, own_half = ((x + 1) // 2) % 2, x // 2

    def piece(i):
        return src.at[own_source, own_half, i, pl.ds(0, HALF)]

    def own_from_psi(i):
        return pltpu.make_async_copy(psi_hbm.at[pl.ds(LINES * i, HALF), 0], piece(i), own_sem.at[i])

    def own_from_half(i):
        return pltpu.make_async_copy(half_hbm.at[i, pl.ds(0, HALF)], piece(i), own_sem.at[i])

    @pl.when(zh == 0)
    def _():
        @pl.when(x < 2)
        def _():
            for i in range(THICK):
                own_from_psi(i).start()

        @pl.when(x >= 2)
        def _():
            for i in range(THICK):
                own_from_half(i).start()

    lane = lax.broadcasted_iota(jnp.int32, (HALF // 7, 128), 1)

    def to_rows(rows, at):
        flat = [rows(b) for b in range(7)]
        for a in range(8):
            if a == 0:
                value = flat[0]
            else:
                below = flat[a] if a < 7 else jnp.zeros_like(flat[0])
                value = pltpu.roll(jnp.where(lane < 128 - 16 * a, below, flat[a - 1]), 16 * a, 1)
            at(a, value)

    for buffer in (r_in, h_in):
        for share in range(SHARES):
            rows = slice(BLOCK * share + USED, BLOCK * (share + 1))
            buffer[rows, :] = jnp.zeros((BLOCK - USED, 128), f32)
    load_psi.wait()
    for i in range(THICK):
        for h in range(2):
            def put(a, value, i=i, h=h):
                psi_y[pl.ds(NG * i + 56 * h + a, 7, stride=8), :] = value

            to_rows(lambda b, i=i, h=h: psi[pl.ds(LINES * i + HALF * h + b, 7, stride=7), :], put)
    for k in range(THICK):
        kern[k] = kernel_tile(THICK * me + k, (128, 128))
    load_tab.wait()

    @pl.when(zh == 0)
    def _():
        for i in range(THICK):
            own_from_psi(i).wait()

    pl.semaphore_wait(barrier, len(peers))

    def along_z(d, i):
        return send(piece(i), piece(i), zs.at[d - 1, i], zr.at[i], at_z(d))

    def along_x(d, i):
        return send(piece(i), piece(i), xs.at[d - 1, i], xr.at[i], at_x(d))

    def from_origin(act):
        @pl.when(zh == 0)
        def _():
            for i in range(THICK):
                for d in (2, 3, 1) if i < 2 else (3, 1):
                    act(along_z(d, i))

    def passed_on(i, act):
        if i >= 2:
            @pl.when(zh == (1 if i % 2 == 0 else 3))
            def _():
                act(along_z(1 if i % 2 == 0 else 3, i))

    def block(buffer, share, start, count):
        return buffer.at[pl.ds(BLOCK * share + start, count)]

    def exchange(source, target, send_sem, recv_sem, d, i):
        return send(
            block(source, (me + d) % SHARES, ROWS * i, ROWS), block(target, me, ROWS * i, ROWS),
            send_sem, recv_sem, at_plane(d),
        )

    def keep(source, target):
        rows = pl.ds(pl.multiple_of(BLOCK * me, 8), BLOCK)
        target[rows, :] = source[rows, :]

    def forward(i):
        rows = slice(NG * i, NG * (i + 1))
        for j in range(2):
            for h in range(2):
                def put(a, value, j=j, h=h):
                    src_y[j, pl.ds(NG * i + 56 * h + a, 7, stride=8), :] = value

                to_rows(lambda b, j=j, h=h: src[j, h, i, pl.ds(b, 7, stride=7), :], put)
        field = psi_y[rows, :]
        density = jnp.concatenate([field * src_y[0, rows, :], field * src_y[1, rows, :]], axis=1)
        values = from_right(density, tab[0], tab[1])
        values = jnp.concatenate([values[:, 0:128], values[:, 128:256]], axis=0)
        values = from_left(tab[2, :, 0 : 2 * NG], tab[3, :, 0 : 2 * NG], values)
        for share in range(SHARES):
            start = BLOCK * share + ROWS * i
            s_out[start : start + ROWS, :] = values[16 * share : 16 * share + ROWS, :]

    from_origin(lambda copy: copy.start())
    for step in range(THICK + LAG):
        if step < THICK:
            @pl.when(zh != 0)
            def _():
                along_z(1, step).wait_recv()

            passed_on(step, lambda copy: copy.start())
            for d in (1, 3, 2):
                along_x(d, step).start()
        if step >= LAG:
            i = step - LAG
            gone = s_out.at[pl.ds(0, 3 * HALF)]
            send(gone, gone, xs.at[0, i], xr.at[i], at_x(1)).wait_recv()
            forward(i)
            for d in ORDER:
                exchange(s_out, r_in, fs, fr, d, i).start()
    keep(s_out, r_in)
    whole = pl.ds(0, (SHARES - 1) * USED)
    send(s_out.at[whole], r_in.at[whole], fs, fr, at_plane(1)).wait_recv()

    def middle(waves):
        columns = []
        for k in waves:
            columns.append(jnp.concatenate(
                [r_in[pl.ds(k, 128, stride=ROWS), :], r_in[pl.ds(THICK + k, 128, stride=ROWS), :]], axis=0))
        spectrum = from_left(tab[4], tab[5], jnp.concatenate(columns, axis=1))
        factor = jnp.concatenate([kern[k] for k in waves], axis=1)
        spectrum = spectrum * jnp.concatenate([factor, factor], axis=0)
        result = from_left(tab[6], tab[7], spectrum)
        for place, k in enumerate(waves):
            lanes = slice(128 * place, 128 * (place + 1))
            g_out[pl.ds(k, 128, stride=ROWS), :] = result[0:128, lanes]
            g_out[pl.ds(THICK + k, 128, stride=ROWS), :] = result[128:256, lanes]

    for waves in ((0, 1), (2, 3), (4, 5), (6,)):
        middle(waves)

    for i in reversed(range(THICK)):
        for d in ORDER:
            exchange(g_out, h_in, bs, br.at[i], d, i).start()
    keep(g_out, h_in)

    def result(i):
        rows = pl.ds(LINES * i, LINES)
        return pltpu.make_async_copy(psi.at[rows], out.at[rows, 0], own_sem.at[i])

    out_lane = lax.broadcasted_iota(jnp.int32, (NG // 8, 128), 1)

    def back(i):
        columns = [h_in[BLOCK * q + ROWS * i : BLOCK * q + ROWS * i + 16, :] for q in range(SHARES)]
        values = from_left(tab[8, 0 : 2 * NG], tab[9, 0 : 2 * NG], jnp.concatenate(columns, axis=0))
        both = jnp.concatenate([values[0:NG], values[NG : 2 * NG]], axis=1)
        potential = from_right(both, tab[10], tab[11])
        rows = slice(NG * i, NG * (i + 1))
        psi_y[rows, :] = potential[:, 0:128] * src_y[0, rows, :] + potential[:, 128:256] * src_y[1, rows, :]
        turned = []
        for a in range(8):
            value = psi_y[pl.ds(NG * i + a, NG // 8, stride=8), :]
            turned.append(pltpu.roll(value, 128 - 16 * a, 1) if a else value)
        for b in range(7):
            value = jnp.where(out_lane < NG - 16 * b, turned[b], turned[b + 1])
            psi[pl.ds(LINES * i + b, NG // 8, stride=7), :] = value

    for i in reversed(range(THICK)):
        rows = pl.ds(0, (SHARES - 1) * ROWS)
        send(g_out.at[rows], h_in.at[rows], bs, br.at[i], at_plane(1)).wait_recv()
        back(i)
        result(i).start()

    for i in range(THICK):
        result(i).wait()
    from_origin(lambda copy: copy.wait_send())
    for i in range(THICK):
        passed_on(i, lambda copy: copy.wait_send())
        for d in (1, 3, 2):
            along_x(d, i).wait_send()
    send(s_out.at[whole], r_in.at[whole], fs, fr, at_plane(1)).wait_send()
    send(g_out.at[whole], h_in.at[whole], bs, br.at[0], at_plane(1)).wait_send()


def on_device(orbitals):
    table = jnp.asarray(tables())
    field = orbitals.reshape(THICK * LINES, 1, 128)
    dma = pltpu.SemaphoreType.DMA
    vmem = pltpu.VMEM
    anywhere = pl.BlockSpec(memory_space=pl.ANY)
    half = pl.pallas_call(
        spread,
        out_shape=jax.ShapeDtypeStruct((THICK, 56, 128), f32),
        in_specs=[anywhere],
        out_specs=anywhere,
        scratch_shapes=[dma((THICK,)), dma((THICK,))],
        compiler_params=pltpu.CompilerParams(collective_id=1, has_side_effects=True),
    )(field)
    exchanged = vmem((SHARES * BLOCK, 128), f32)
    total = pl.pallas_call(
        body,
        out_shape=jax.ShapeDtypeStruct((THICK * LINES, 1, 128), f32),
        in_specs=[anywhere] * 3,
        out_specs=anywhere,
        scratch_shapes=[
            vmem((THICK * LINES, 128), f32),
            vmem((12, 256, 256), bf16),
            vmem((2, 2, THICK, 56, 128), f32),
            vmem((THICK * NG, 128), f32),
            vmem((2, THICK * NG, 128), f32),
            vmem((THICK, 128, 128), f32),
            exchanged, exchanged, exchanged, exchanged,
            dma((2,)), dma((THICK,)), dma((3, THICK)), dma((THICK,)), dma((3, THICK)), dma((THICK,)),
            dma, dma, dma, dma((THICK,)),
        ],
        compiler_params=pltpu.CompilerParams(collective_id=0, has_side_effects=True),
    )(field, half, table)
    return total.reshape(orbitals.shape)


def solution(mesh):
    spec = P("band", "plane", None)
    return jax.shard_map(on_device, mesh=mesh, in_specs=(spec,), out_specs=spec, check_vma=False)
```

```python
import math

import jax
import jax.numpy as jnp
import ml_dtypes
import numpy as np
from jax import lax
from jax.experimental import pallas as pl
from jax.experimental.pallas import tpu as pltpu
from jax.sharding import PartitionSpec as P

MESH = pl.DeviceIdType.MESH
NG = 112
FLAT = NG * NG
LINES = FLAT // 128
HALF = LINES // 2
EVEN_FIRST = (-1, -3, -5, -7, 1, 3, -2, 5, -4, 7, -6, 2, 4, 6)
ODD_FIRST = (-2, -4, -1, -6, -3, 2, -5, 4, -7, 1, 6, 3, 5, 7)
SHARES = 16
THICK = NG // SHARES
ROWS = 2 * THICK
BLOCK = 112
USED = THICK * ROWS
ORDER = (10, 11, 8, 9, 6, 14, 7, 13, 2, 3, 4, 12, 5, 15, 1)
screen_omega = 0.106
cell_length = 46.93
mixing = 0.25
f32, bf16 = jnp.float32, jnp.bfloat16


def tables():
    index = np.arange(NG)
    angle = (index[:, None] * index[None, :] % NG) * (2.0 * math.pi / NG)
    cos, sin = np.cos(angle), np.sin(angle)
    re, im = slice(0, NG), slice(128, 128 + NG)
    last = np.zeros((256, 256))
    last[re, re], last[im, re] = cos, sin
    last[re, im], last[im, im] = -sin, cos
    last_back = np.zeros((256, 256))
    last_back[re, re], last_back[im, re] = cos, -sin
    last_back[re, im], last_back[im, im] = sin, cos
    second = np.zeros((256, 256))
    second_back = np.zeros((256, 256))
    for share in range(SHARES):
        for part in range(2):
            for k in range(THICK):
                row, wave = 16 * share + THICK * part + k, THICK * share + k
                if part == 0:
                    second[row, 0:NG], second[row, NG : 2 * NG] = cos[wave], sin[wave]
                    second_back[0:NG, row], second_back[NG : 2 * NG, row] = cos[wave], sin[wave]
                else:
                    second[row, 0:NG], second[row, NG : 2 * NG] = -sin[wave], cos[wave]
                    second_back[0:NG, row], second_back[NG : 2 * NG, row] = -sin[wave], cos[wave]
    place = 8 * (index // THICK) + index % THICK
    first = np.zeros((256, 256))
    first_back = np.zeros((256, 256))
    first[re, place], first[re, 128 + place] = cos, sin
    first[im, place], first[im, 128 + place] = -sin, cos
    first_back[place, re], first_back[place, im] = cos, -sin
    first_back[128 + place, re], first_back[128 + place, im] = sin, cos
    both = []
    for table in (last, second, first, first_back, second_back, last_back):
        high = table.astype(ml_dtypes.bfloat16)
        both += [high, (table - high.astype(np.float64)).astype(ml_dtypes.bfloat16)]
    return np.stack(both)


def split(values):
    high = values.astype(bf16)
    return high, (values - high.astype(f32)).astype(bf16)


def dot(a, b):
    return jnp.dot(a, b, preferred_element_type=f32)


def from_left(high, low, values):
    big, small = split(values)
    return dot(high, big) + dot(high, small) + dot(low, big)


def from_right(values, high, low):
    big, small = split(values)
    return dot(big, high) + dot(small, high) + dot(big, low)


def kernel_tile(k_second, shape):
    def wave(index):
        return jnp.where(2 * index < NG, index, index - NG).astype(f32)

    first = wave(lax.broadcasted_iota(jnp.int32, shape, 0))
    last = wave(lax.broadcasted_iota(jnp.int32, shape, 1))
    second = wave(jnp.full(shape, k_second, jnp.int32))
    gsquare = (first * first + second * second + last * last) * (2.0 * math.pi / cell_length) ** 2
    safe = jnp.where(gsquare > 0, gsquare, 1.0)
    values = 4.0 * math.pi / safe * (1.0 - jnp.exp(-safe / (4.0 * screen_omega * screen_omega)))
    values = jnp.where(gsquare > 0, values, math.pi / (screen_omega * screen_omega))
    return values * (-mixing / float(NG) ** 3)


def kernel_axes():
    band = lax.axis_index("band")
    return band % 4, band // 4, lax.axis_index("plane")


def send(source, target, send_sem, recv_sem, device):
    return pltpu.make_async_remote_copy(
        src_ref=source, dst_ref=target, send_sem=send_sem, recv_sem=recv_sem,
        device_id=device, device_id_type=MESH,
    )


def spread(psi_hbm, half_hbm, send_sem, recv_sem):
    x, zh, me = kernel_axes()

    def half(i):
        return send(
            psi_hbm.at[pl.ds(LINES * i + HALF, HALF), 0], half_hbm.at[i, pl.ds(0, HALF)],
            send_sem.at[i], recv_sem.at[i], (zh * 4 + 3 - x, me),
        )

    @pl.when(zh == 0)
    def _():
        barrier = pltpu.get_barrier_semaphore()
        pl.semaphore_signal(barrier, inc=1, device_id=(zh * 4 + 3 - x, me), device_id_type=MESH)
        pl.semaphore_wait(barrier, 1)

        @pl.when(x < 2)
        def _():
            for i in range(THICK):
                half(i).start()
            for i in range(THICK):
                half(i).wait_send()

        @pl.when(x >= 2)
        def _():
            for i in range(THICK):
                half(i).wait_recv()


def body(
    psi_hbm, half_hbm, tab_hbm, out,
    psi, tab, src, psi_y, src_y, kern, s_out, r_in, g_out, h_in,
    load_sem, own_sem, zs, zr, xs, xr, fs, fr, bs, br,
):
    x, zh, me = kernel_axes()
    band = zh * 4 + x

    def at_x(d):
        return (zh * 4 + (x + d) % 4, me)

    def at_z(d):
        return (((zh + d) % 4) * 4 + x, me)

    def at_plane(d):
        return (band, (me + d) % SHARES)

    barrier = pltpu.get_barrier_semaphore()
    peers = [at_x(d) for d in (1, 2, 3)] + [at_z(d) for d in (1, 2, 3)]
    peers += [at_plane(d) for d in range(1, SHARES)]
    for peer in peers:
        pl.semaphore_signal(barrier, inc=1, device_id=peer, device_id_type=MESH)

    load_psi = pltpu.make_async_copy(psi_hbm.at[:, 0], psi, load_sem.at[0])
    load_psi.start()
    load_tab = pltpu.make_async_copy(tab_hbm, tab, load_sem.at[1])
    load_tab.start()

    own_source, own_half = ((x + 1) // 2) % 2, x // 2

    def piece(i):
        return src.at[own_source, own_half, i, pl.ds(0, HALF)]

    def own_from_psi(i):
        return pltpu.make_async_copy(psi_hbm.at[pl.ds(LINES * i, HALF), 0], piece(i), own_sem.at[i])

    def own_from_half(i):
        return pltpu.make_async_copy(half_hbm.at[i, pl.ds(0, HALF)], piece(i), own_sem.at[i])

    @pl.when(zh == 0)
    def _():
        @pl.when(x < 2)
        def _():
            for i in range(THICK):
                own_from_psi(i).start()

        @pl.when(x >= 2)
        def _():
            for i in range(THICK):
                own_from_half(i).start()

    lane = lax.broadcasted_iota(jnp.int32, (HALF // 7, 128), 1)

    def to_rows(rows, at):
        flat = [rows(b) for b in range(7)]
        for a in range(8):
            if a == 0:
                value = flat[0]
            else:
                below = flat[a] if a < 7 else jnp.zeros_like(flat[0])
                value = pltpu.roll(jnp.where(lane < 128 - 16 * a, below, flat[a - 1]), 16 * a, 1)
            at(a, value)

    for buffer in (r_in, h_in):
        for share in range(SHARES):
            rows = slice(BLOCK * share + USED, BLOCK * (share + 1))
            buffer[rows, :] = jnp.zeros((BLOCK - USED, 128), f32)
    load_psi.wait()
    for i in range(THICK):
        for h in range(2):
            def put(a, value, i=i, h=h):
                psi_y[pl.ds(NG * i + 56 * h + a, 7, stride=8), :] = value

            to_rows(lambda b, i=i, h=h: psi[pl.ds(LINES * i + HALF * h + b, 7, stride=7), :], put)
    for k in range(THICK):
        kern[k] = kernel_tile(THICK * me + k, (128, 128))
    load_tab.wait()

    @pl.when(zh == 0)
    def _():
        for i in range(THICK):
            own_from_psi(i).wait()

    pl.semaphore_wait(barrier, len(peers))

    def along_z(d, i):
        return send(piece(i), piece(i), zs.at[d - 1, i], zr.at[i], at_z(d))

    def along_x(d, i):
        return send(piece(i), piece(i), xs.at[d - 1, i], xr.at[i], at_x(d))

    def from_origin(act):
        @pl.when(zh == 0)
        def _():
            for i in (0, 2, 4, 6):
                act(along_z(2, i))
            for i in (1, 3, 5):
                for d in (3, 1):
                    act(along_z(d, i))

    def passed_on(i, act):
        relay = 2 if i % 2 == 0 else 3 if i == 3 else 1

        @pl.when(zh == relay)
        def _():
            for d in (1, 3) if relay == 2 else (relay,):
                act(along_z(d, i))

    def block(buffer, share, start, count):
        return buffer.at[pl.ds(BLOCK * share + start, count)]

    def exchange(source, target, send_sem, recv_sem, d, i):
        return send(
            block(source, (me + d) % SHARES, ROWS * i, ROWS), block(target, me, ROWS * i, ROWS),
            send_sem, recv_sem, at_plane(d),
        )

    def keep(source, target):
        rows = pl.ds(pl.multiple_of(BLOCK * me, 8), BLOCK)
        target[rows, :] = source[rows, :]

    def forward(i):
        rows = slice(NG * i, NG * (i + 1))
        for j in range(2):
            for h in range(2):
                def put(a, value, j=j, h=h):
                    src_y[j, pl.ds(NG * i + 56 * h + a, 7, stride=8), :] = value

                to_rows(lambda b, j=j, h=h: src[j, h, i, pl.ds(b, 7, stride=7), :], put)
        field = psi_y[rows, :]
        density = jnp.concatenate([field * src_y[0, rows, :], field * src_y[1, rows, :]], axis=1)
        values = from_right(density, tab[0], tab[1])
        values = jnp.concatenate([values[:, 0:128], values[:, 128:256]], axis=0)
        values = from_left(tab[2, :, 0 : 2 * NG], tab[3, :, 0 : 2 * NG], values)
        for share in range(SHARES):
            start = BLOCK * share + ROWS * i
            s_out[start : start + ROWS, :] = values[16 * share : 16 * share + ROWS, :]

    from_origin(lambda copy: copy.start())

    def pass_on(i):
        @pl.when(zh != 0)
        def _():
            along_z(1, i).wait_recv()

        passed_on(i, lambda copy: copy.start())
        for d in (1, 3, 2):
            along_x(d, i).start()

    def take(i):
        gone = s_out.at[pl.ds(0, 3 * HALF)]
        send(gone, gone, xs.at[0, i], xr.at[i], at_x(1)).wait_recv()
        forward(i)
        for d in ORDER:
            exchange(s_out, r_in, fs, fr, d, i).start()

    def in_order(steps):
        for step in steps:
            (pass_on if step < 0 else take)(abs(step) - 1)

    @pl.when(zh == 2)
    def _():
        in_order(EVEN_FIRST)

    @pl.when(zh != 2)
    def _():
        in_order(ODD_FIRST)

    keep(s_out, r_in)
    whole = pl.ds(0, (SHARES - 1) * USED)
    send(s_out.at[whole], r_in.at[whole], fs, fr, at_plane(1)).wait_recv()

    def middle(waves):
        columns = []
        for k in waves:
            columns.append(jnp.concatenate(
                [r_in[pl.ds(k, 128, stride=ROWS), :], r_in[pl.ds(THICK + k, 128, stride=ROWS), :]], axis=0))
        spectrum = from_left(tab[4], tab[5], jnp.concatenate(columns, axis=1))
        factor = jnp.concatenate([kern[k] for k in waves], axis=1)
        spectrum = spectrum * jnp.concatenate([factor, factor], axis=0)
        result = from_left(tab[6], tab[7], spectrum)
        for place, k in enumerate(waves):
            lanes = slice(128 * place, 128 * (place + 1))
            g_out[pl.ds(k, 128, stride=ROWS), :] = result[0:128, lanes]
            g_out[pl.ds(THICK + k, 128, stride=ROWS), :] = result[128:256, lanes]

    for waves in ((0, 1), (2, 3), (4, 5), (6,)):
        middle(waves)

    for i in reversed(range(THICK)):
        for d in ORDER:
            exchange(g_out, h_in, bs, br.at[i], d, i).start()
    keep(g_out, h_in)

    def result(i):
        rows = pl.ds(LINES * i, LINES)
        return pltpu.make_async_copy(psi.at[rows], out.at[rows, 0], own_sem.at[i])

    out_lane = lax.broadcasted_iota(jnp.int32, (NG // 8, 128), 1)

    def back(i):
        columns = [h_in[BLOCK * q + ROWS * i : BLOCK * q + ROWS * i + 16, :] for q in range(SHARES)]
        values = from_left(tab[8, 0 : 2 * NG], tab[9, 0 : 2 * NG], jnp.concatenate(columns, axis=0))
        both = jnp.concatenate([values[0:NG], values[NG : 2 * NG]], axis=1)
        potential = from_right(both, tab[10], tab[11])
        rows = slice(NG * i, NG * (i + 1))
        psi_y[rows, :] = potential[:, 0:128] * src_y[0, rows, :] + potential[:, 128:256] * src_y[1, rows, :]
        turned = []
        for a in range(8):
            value = psi_y[pl.ds(NG * i + a, NG // 8, stride=8), :]
            turned.append(pltpu.roll(value, 128 - 16 * a, 1) if a else value)
        for b in range(7):
            value = jnp.where(out_lane < NG - 16 * b, turned[b], turned[b + 1])
            psi[pl.ds(LINES * i + b, NG // 8, stride=7), :] = value

    for i in reversed(range(THICK)):
        rows = pl.ds(0, (SHARES - 1) * ROWS)
        send(g_out.at[rows], h_in.at[rows], bs, br.at[i], at_plane(1)).wait_recv()
        back(i)
        result(i).start()

    for i in range(THICK):
        result(i).wait()
    from_origin(lambda copy: copy.wait_send())
    for i in range(THICK):
        passed_on(i, lambda copy: copy.wait_send())
        for d in (1, 3, 2):
            along_x(d, i).wait_send()
    send(s_out.at[whole], r_in.at[whole], fs, fr, at_plane(1)).wait_send()
    send(g_out.at[whole], h_in.at[whole], bs, br.at[0], at_plane(1)).wait_send()


def on_device(orbitals):
    table = jnp.asarray(tables())
    field = orbitals.reshape(THICK * LINES, 1, 128)
    dma = pltpu.SemaphoreType.DMA
    vmem = pltpu.VMEM
    anywhere = pl.BlockSpec(memory_space=pl.ANY)
    half = pl.pallas_call(
        spread,
        out_shape=jax.ShapeDtypeStruct((THICK, 56, 128), f32),
        in_specs=[anywhere],
        out_specs=anywhere,
        scratch_shapes=[dma((THICK,)), dma((THICK,))],
        compiler_params=pltpu.CompilerParams(collective_id=1, has_side_effects=True),
    )(field)
    exchanged = vmem((SHARES * BLOCK, 128), f32)
    total = pl.pallas_call(
        body,
        out_shape=jax.ShapeDtypeStruct((THICK * LINES, 1, 128), f32),
        in_specs=[anywhere] * 3,
        out_specs=anywhere,
        scratch_shapes=[
            vmem((THICK * LINES, 128), f32),
            vmem((12, 256, 256), bf16),
            vmem((2, 2, THICK, 56, 128), f32),
            vmem((THICK * NG, 128), f32),
            vmem((2, THICK * NG, 128), f32),
            vmem((THICK, 128, 128), f32),
            exchanged, exchanged, exchanged, exchanged,
            dma((2,)), dma((THICK,)), dma((3, THICK)), dma((THICK,)), dma((3, THICK)), dma((THICK,)),
            dma, dma, dma, dma((THICK,)),
        ],
        compiler_params=pltpu.CompilerParams(collective_id=0, has_side_effects=True),
    )(field, half, table)
    return total.reshape(orbitals.shape)


def solution(mesh):
    spec = P("band", "plane", None)
    return jax.shard_map(on_device, mesh=mesh, in_specs=(spec,), out_specs=spec, check_vma=False)
```

```python
import math

import jax
import jax.numpy as jnp
import ml_dtypes
import numpy as np
from jax import lax
from jax.experimental import pallas as pl
from jax.experimental.pallas import tpu as pltpu
from jax.sharding import PartitionSpec as P

MESH = pl.DeviceIdType.MESH
NG = 112
FLAT = NG * NG
LINES = FLAT // 128
HALF = LINES // 2
EVEN_FIRST = (-1, -3, -5, -7, 1, 3, -2, 5, -4, 7, -6, 2, 4, 6)
ODD_FIRST = (-2, -4, -1, -6, -3, 2, -5, 4, -7, 1, 6, 3, 5, 7)
SHARES = 16
THICK = NG // SHARES
ROWS = 2 * THICK
BLOCK = 112
USED = THICK * ROWS
ORDER = (10, 11, 8, 9, 6, 14, 7, 13, 2, 3, 4, 12, 5, 15, 1)
screen_omega = 0.106
cell_length = 46.93
mixing = 0.25
f32, bf16 = jnp.float32, jnp.bfloat16


def tables():
    index = np.arange(NG)
    angle = (index[:, None] * index[None, :] % NG) * (2.0 * math.pi / NG)
    cos, sin = np.cos(angle), np.sin(angle)
    re, im = slice(0, NG), slice(128, 128 + NG)
    last = np.zeros((256, 256))
    last[re, re], last[im, re] = cos, sin
    last[re, im], last[im, im] = -sin, cos
    last_back = np.zeros((256, 256))
    last_back[re, re], last_back[im, re] = cos, -sin
    last_back[re, im], last_back[im, im] = sin, cos
    second = np.zeros((256, 256))
    second_back = np.zeros((256, 256))
    for share in range(SHARES):
        for part in range(2):
            for k in range(THICK):
                row, wave = 16 * share + THICK * part + k, THICK * share + k
                if part == 0:
                    second[row, 0:NG], second[row, NG : 2 * NG] = cos[wave], sin[wave]
                    second_back[0:NG, row], second_back[NG : 2 * NG, row] = cos[wave], sin[wave]
                else:
                    second[row, 0:NG], second[row, NG : 2 * NG] = -sin[wave], cos[wave]
                    second_back[0:NG, row], second_back[NG : 2 * NG, row] = -sin[wave], cos[wave]
    place = 8 * (index // THICK) + index % THICK
    first = np.zeros((256, 256))
    first_back = np.zeros((256, 256))
    first[re, place], first[re, 128 + place] = cos, sin
    first[im, place], first[im, 128 + place] = -sin, cos
    first_back[place, re], first_back[place, im] = cos, -sin
    first_back[128 + place, re], first_back[128 + place, im] = sin, cos
    both = []
    for table in (last, second, first, first_back, second_back, last_back):
        high = table.astype(ml_dtypes.bfloat16)
        both += [high, (table - high.astype(np.float64)).astype(ml_dtypes.bfloat16)]
    return np.stack(both)


def split(values):
    high = values.astype(bf16)
    return high, (values - high.astype(f32)).astype(bf16)


def dot(a, b):
    return jnp.dot(a, b, preferred_element_type=f32)


def from_left(high, low, values):
    big, small = split(values)
    return dot(high, big) + dot(high, small) + dot(low, big)


def from_right(values, high, low):
    big, small = split(values)
    return dot(big, high) + dot(small, high) + dot(big, low)


def kernel_tile(k_second, shape):
    def wave(index):
        return jnp.where(2 * index < NG, index, index - NG).astype(f32)

    first = wave(lax.broadcasted_iota(jnp.int32, shape, 0))
    last = wave(lax.broadcasted_iota(jnp.int32, shape, 1))
    second = wave(jnp.full(shape, k_second, jnp.int32))
    gsquare = (first * first + second * second + last * last) * (2.0 * math.pi / cell_length) ** 2
    safe = jnp.where(gsquare > 0, gsquare, 1.0)
    values = 4.0 * math.pi / safe * (1.0 - jnp.exp(-safe / (4.0 * screen_omega * screen_omega)))
    values = jnp.where(gsquare > 0, values, math.pi / (screen_omega * screen_omega))
    return values * (-mixing / float(NG) ** 3)


def kernel_axes():
    band = lax.axis_index("band")
    return band % 4, band // 4, lax.axis_index("plane")


def send(source, target, send_sem, recv_sem, device):
    return pltpu.make_async_remote_copy(
        src_ref=source, dst_ref=target, send_sem=send_sem, recv_sem=recv_sem,
        device_id=device, device_id_type=MESH,
    )


def spread(psi_hbm, half_hbm, send_sem, recv_sem):
    x, zh, me = kernel_axes()

    def half(i):
        return send(
            psi_hbm.at[pl.ds(LINES * i + HALF, HALF), 0], half_hbm.at[i, pl.ds(0, HALF)],
            send_sem.at[i], recv_sem.at[i], (zh * 4 + 3 - x, me),
        )

    @pl.when(zh == 0)
    def _():
        barrier = pltpu.get_barrier_semaphore()
        pl.semaphore_signal(barrier, inc=1, device_id=(zh * 4 + 3 - x, me), device_id_type=MESH)
        pl.semaphore_wait(barrier, 1)

        @pl.when(x < 2)
        def _():
            for i in range(THICK):
                half(i).start()
            for i in range(THICK):
                half(i).wait_send()

        @pl.when(x >= 2)
        def _():
            for i in range(THICK):
                half(i).wait_recv()


def body(
    psi_hbm, half_hbm, tab_hbm, out,
    psi, tab, src, psi_y, src_y, kern, s_out, r_in, g_out, h_in,
    load_sem, own_sem, zs, zr, xs, xr, fs, fr, bs, br,
):
    x, zh, me = kernel_axes()
    band = zh * 4 + x

    def at_x(d):
        return (zh * 4 + (x + d) % 4, me)

    def at_z(d):
        return (((zh + d) % 4) * 4 + x, me)

    def at_plane(d):
        return (band, (me + d) % SHARES)

    barrier = pltpu.get_barrier_semaphore()
    peers = [at_x(d) for d in (1, 2, 3)] + [at_z(d) for d in (1, 2, 3)]
    peers += [at_plane(d) for d in range(1, SHARES)]
    for peer in peers:
        pl.semaphore_signal(barrier, inc=1, device_id=peer, device_id_type=MESH)

    load_psi = pltpu.make_async_copy(psi_hbm.at[:, 0], psi, load_sem.at[0])
    load_psi.start()
    load_tab = pltpu.make_async_copy(tab_hbm, tab, load_sem.at[1])
    load_tab.start()

    own_source, own_half = ((x + 1) // 2) % 2, x // 2

    def piece(i):
        return src.at[own_source, own_half, i, pl.ds(0, HALF)]

    def own_from_psi(i):
        return pltpu.make_async_copy(psi_hbm.at[pl.ds(LINES * i, HALF), 0], piece(i), own_sem.at[i])

    def own_from_half(i):
        return pltpu.make_async_copy(half_hbm.at[i, pl.ds(0, HALF)], piece(i), own_sem.at[i])

    @pl.when(zh == 0)
    def _():
        @pl.when(x < 2)
        def _():
            for i in range(THICK):
                own_from_psi(i).start()

        @pl.when(x >= 2)
        def _():
            for i in range(THICK):
                own_from_half(i).start()

    lane = lax.broadcasted_iota(jnp.int32, (HALF // 7, 128), 1)

    def to_rows(rows, at):
        flat = [rows(b) for b in range(7)]
        for a in range(8):
            if a == 0:
                value = flat[0]
            else:
                below = flat[a] if a < 7 else jnp.zeros_like(flat[0])
                value = pltpu.roll(jnp.where(lane < 128 - 16 * a, below, flat[a - 1]), 16 * a, 1)
            at(a, value)

    def along_z(d, i):
        return send(piece(i), piece(i), zs.at[d - 1, i], zr.at[i], at_z(d))

    def along_x(d, i):
        return send(piece(i), piece(i), xs.at[d - 1, i], xr.at[i], at_x(d))

    def from_origin(act):
        @pl.when(zh == 0)
        def _():
            for i in (0, 2, 4, 6):
                act(along_z(2, i))
            for i in (1, 3, 5):
                for d in (3, 1):
                    act(along_z(d, i))

    def passed_on(i, act):
        relay = 2 if i % 2 == 0 else 3 if i == 3 else 1

        @pl.when(zh == relay)
        def _():
            for d in (1, 3) if relay == 2 else (relay,):
                act(along_z(d, i))

    @pl.when(zh == 0)
    def _():
        for i in range(THICK):
            own_from_psi(i).wait()
        pl.semaphore_wait(barrier, len(peers))

    from_origin(lambda copy: copy.start())

    for buffer in (r_in, h_in):
        for share in range(SHARES):
            rows = slice(BLOCK * share + USED, BLOCK * (share + 1))
            buffer[rows, :] = jnp.zeros((BLOCK - USED, 128), f32)
    load_psi.wait()
    for i in range(THICK):
        for h in range(2):
            def put(a, value, i=i, h=h):
                psi_y[pl.ds(NG * i + 56 * h + a, 7, stride=8), :] = value

            to_rows(lambda b, i=i, h=h: psi[pl.ds(LINES * i + HALF * h + b, 7, stride=7), :], put)
    for k in range(THICK):
        kern[k] = kernel_tile(THICK * me + k, (128, 128))
    load_tab.wait()

    @pl.when(zh != 0)
    def _():
        pl.semaphore_wait(barrier, len(peers))

    def block(buffer, share, start, count):
        return buffer.at[pl.ds(BLOCK * share + start, count)]

    def exchange(source, target, send_sem, recv_sem, d, i):
        return send(
            block(source, (me + d) % SHARES, ROWS * i, ROWS), block(target, me, ROWS * i, ROWS),
            send_sem, recv_sem, at_plane(d),
        )

    def keep(source, target):
        rows = pl.ds(pl.multiple_of(BLOCK * me, 8), BLOCK)
        target[rows, :] = source[rows, :]

    def forward(i):
        rows = slice(NG * i, NG * (i + 1))
        for j in range(2):
            for h in range(2):
                def put(a, value, j=j, h=h):
                    src_y[j, pl.ds(NG * i + 56 * h + a, 7, stride=8), :] = value

                to_rows(lambda b, j=j, h=h: src[j, h, i, pl.ds(b, 7, stride=7), :], put)
        field = psi_y[rows, :]
        density = jnp.concatenate([field * src_y[0, rows, :], field * src_y[1, rows, :]], axis=1)
        values = from_right(density, tab[0], tab[1])
        values = jnp.concatenate([values[:, 0:128], values[:, 128:256]], axis=0)
        values = from_left(tab[2, :, 0 : 2 * NG], tab[3, :, 0 : 2 * NG], values)
        for share in range(SHARES):
            start = BLOCK * share + ROWS * i
            s_out[start : start + ROWS, :] = values[16 * share : 16 * share + ROWS, :]

    def pass_on(i):
        @pl.when(zh != 0)
        def _():
            along_z(1, i).wait_recv()

        passed_on(i, lambda copy: copy.start())
        for d in (1, 3, 2):
            along_x(d, i).start()

    def take(i):
        gone = s_out.at[pl.ds(0, 3 * HALF)]
        send(gone, gone, xs.at[0, i], xr.at[i], at_x(1)).wait_recv()
        forward(i)
        for d in ORDER:
            exchange(s_out, r_in, fs, fr, d, i).start()

    def in_order(steps):
        for step in steps:
            (pass_on if step < 0 else take)(abs(step) - 1)

    @pl.when(zh == 2)
    def _():
        in_order(EVEN_FIRST)

    @pl.when(zh != 2)
    def _():
        in_order(ODD_FIRST)

    keep(s_out, r_in)
    whole = pl.ds(0, (SHARES - 1) * USED)
    send(s_out.at[whole], r_in.at[whole], fs, fr, at_plane(1)).wait_recv()

    def middle(waves):
        columns = []
        for k in waves:
            columns.append(jnp.concatenate(
                [r_in[pl.ds(k, 128, stride=ROWS), :], r_in[pl.ds(THICK + k, 128, stride=ROWS), :]], axis=0))
        spectrum = from_left(tab[4], tab[5], jnp.concatenate(columns, axis=1))
        factor = jnp.concatenate([kern[k] for k in waves], axis=1)
        spectrum = spectrum * jnp.concatenate([factor, factor], axis=0)
        result = from_left(tab[6], tab[7], spectrum)
        for place, k in enumerate(waves):
            lanes = slice(128 * place, 128 * (place + 1))
            g_out[pl.ds(k, 128, stride=ROWS), :] = result[0:128, lanes]
            g_out[pl.ds(THICK + k, 128, stride=ROWS), :] = result[128:256, lanes]

    for waves in ((0, 1), (2, 3), (4, 5), (6,)):
        middle(waves)

    for i in reversed(range(THICK)):
        for d in ORDER:
            exchange(g_out, h_in, bs, br.at[i], d, i).start()
    keep(g_out, h_in)

    def result(i):
        rows = pl.ds(LINES * i, LINES)
        return pltpu.make_async_copy(psi.at[rows], out.at[rows, 0], own_sem.at[i])

    out_lane = lax.broadcasted_iota(jnp.int32, (NG // 8, 128), 1)

    def back(i):
        columns = [h_in[BLOCK * q + ROWS * i : BLOCK * q + ROWS * i + 16, :] for q in range(SHARES)]
        values = from_left(tab[8, 0 : 2 * NG], tab[9, 0 : 2 * NG], jnp.concatenate(columns, axis=0))
        both = jnp.concatenate([values[0:NG], values[NG : 2 * NG]], axis=1)
        potential = from_right(both, tab[10], tab[11])
        rows = slice(NG * i, NG * (i + 1))
        psi_y[rows, :] = potential[:, 0:128] * src_y[0, rows, :] + potential[:, 128:256] * src_y[1, rows, :]
        turned = []
        for a in range(8):
            value = psi_y[pl.ds(NG * i + a, NG // 8, stride=8), :]
            turned.append(pltpu.roll(value, 128 - 16 * a, 1) if a else value)
        for b in range(7):
            value = jnp.where(out_lane < NG - 16 * b, turned[b], turned[b + 1])
            out[pl.ds(LINES * i + b, NG // 8, stride=7), 0, :] = value

    for i in reversed(range(THICK)):
        rows = pl.ds(0, (SHARES - 1) * ROWS)
        send(g_out.at[rows], h_in.at[rows], bs, br.at[i], at_plane(1)).wait_recv()
        back(i)

    from_origin(lambda copy: copy.wait_send())
    for i in range(THICK):
        passed_on(i, lambda copy: copy.wait_send())
        for d in (1, 3, 2):
            along_x(d, i).wait_send()
    send(s_out.at[whole], r_in.at[whole], fs, fr, at_plane(1)).wait_send()
    send(g_out.at[whole], h_in.at[whole], bs, br.at[0], at_plane(1)).wait_send()


def on_device(orbitals):
    table = jnp.asarray(tables())
    field = orbitals.reshape(THICK * LINES, 1, 128)
    dma = pltpu.SemaphoreType.DMA
    vmem = pltpu.VMEM
    anywhere = pl.BlockSpec(memory_space=pl.ANY)
    half = pl.pallas_call(
        spread,
        out_shape=jax.ShapeDtypeStruct((THICK, 56, 128), f32),
        in_specs=[anywhere],
        out_specs=anywhere,
        scratch_shapes=[dma((THICK,)), dma((THICK,))],
        compiler_params=pltpu.CompilerParams(collective_id=1, has_side_effects=True),
    )(field)
    exchanged = vmem((SHARES * BLOCK, 128), f32)
    total = pl.pallas_call(
        body,
        out_shape=pltpu.VMEM((THICK * LINES, 1, 128), f32),
        in_specs=[anywhere] * 3,
        out_specs=pl.BlockSpec(memory_space=vmem),
        scratch_shapes=[
            vmem((THICK * LINES, 128), f32),
            vmem((12, 256, 256), bf16),
            vmem((2, 2, THICK, 56, 128), f32),
            vmem((THICK * NG, 128), f32),
            vmem((2, THICK * NG, 128), f32),
            vmem((THICK, 128, 128), f32),
            exchanged, exchanged, exchanged, exchanged,
            dma((2,)), dma((THICK,)), dma((3, THICK)), dma((THICK,)), dma((3, THICK)), dma((THICK,)),
            dma, dma, dma, dma((THICK,)),
        ],
        compiler_params=pltpu.CompilerParams(collective_id=0, has_side_effects=True),
    )(field, half, table)
    return total.reshape(orbitals.shape)


def solution(mesh):
    spec = P("band", "plane", None)
    return jax.shard_map(on_device, mesh=mesh, in_specs=(spec,), out_specs=spec, check_vma=False)
```

```python
import math

import jax
import jax.numpy as jnp
import ml_dtypes
import numpy as np
from jax import lax
from jax.experimental import pallas as pl
from jax.experimental.pallas import tpu as pltpu
from jax.sharding import PartitionSpec as P

MESH = pl.DeviceIdType.MESH
NG = 112
FLAT = NG * NG
LINES = FLAT // 128
HALF = LINES // 2
EVEN_FIRST = (-1, -3, -5, -7, 1, 3, -2, 5, -4, 7, -6, 2, 4, 6)
ODD_FIRST = (-2, -4, -1, -6, -3, 2, -5, 4, -7, 1, 6, 3, 5, 7)
SHARES = 16
THICK = NG // SHARES
ROWS = 2 * THICK
BLOCK = 112
USED = THICK * ROWS
ORDER = (10, 11, 8, 9, 6, 14, 7, 13, 2, 3, 4, 12, 5, 15, 1)
screen_omega = 0.106
cell_length = 46.93
mixing = 0.25
f32, bf16 = jnp.float32, jnp.bfloat16


def tables():
    index = np.arange(NG)
    angle = (index[:, None] * index[None, :] % NG) * (2.0 * math.pi / NG)
    cos, sin = np.cos(angle), np.sin(angle)
    re, im = slice(0, NG), slice(128, 128 + NG)
    last = np.zeros((256, 256))
    last[re, re], last[im, re] = cos, sin
    last[re, im], last[im, im] = -sin, cos
    last_back = np.zeros((256, 256))
    last_back[re, re], last_back[im, re] = cos, -sin
    last_back[re, im], last_back[im, im] = sin, cos
    second = np.zeros((256, 256))
    second_back = np.zeros((256, 256))
    for share in range(SHARES):
        for part in range(2):
            for k in range(THICK):
                row, wave = 16 * share + THICK * part + k, THICK * share + k
                if part == 0:
                    second[row, 0:NG], second[row, NG : 2 * NG] = cos[wave], sin[wave]
                    second_back[0:NG, row], second_back[NG : 2 * NG, row] = cos[wave], sin[wave]
                else:
                    second[row, 0:NG], second[row, NG : 2 * NG] = -sin[wave], cos[wave]
                    second_back[0:NG, row], second_back[NG : 2 * NG, row] = -sin[wave], cos[wave]
    place = 8 * (index // THICK) + index % THICK
    first = np.zeros((256, 256))
    first_back = np.zeros((256, 256))
    first[re, place], first[re, 128 + place] = cos, sin
    first[im, place], first[im, 128 + place] = -sin, cos
    first_back[place, re], first_back[place, im] = cos, -sin
    first_back[128 + place, re], first_back[128 + place, im] = sin, cos
    both = []
    for table in (last, second, first, first_back, second_back, last_back):
        high = table.astype(ml_dtypes.bfloat16)
        both += [high, (table - high.astype(np.float64)).astype(ml_dtypes.bfloat16)]
    return np.stack(both)


def split(values):
    high = values.astype(bf16)
    return high, (values - high.astype(f32)).astype(bf16)


def dot(a, b):
    return jnp.dot(a, b, preferred_element_type=f32)


def from_left(high, low, values):
    big, small = split(values)
    return dot(high, big) + dot(high, small) + dot(low, big)


def from_right(values, high, low):
    big, small = split(values)
    return dot(big, high) + dot(small, high) + dot(big, low)


def kernel_tile(k_second, shape):
    def wave(index):
        return jnp.where(2 * index < NG, index, index - NG).astype(f32)

    first = wave(lax.broadcasted_iota(jnp.int32, shape, 0))
    last = wave(lax.broadcasted_iota(jnp.int32, shape, 1))
    second = wave(jnp.full(shape, k_second, jnp.int32))
    gsquare = (first * first + second * second + last * last) * (2.0 * math.pi / cell_length) ** 2
    safe = jnp.where(gsquare > 0, gsquare, 1.0)
    values = 4.0 * math.pi / safe * (1.0 - jnp.exp(-safe / (4.0 * screen_omega * screen_omega)))
    values = jnp.where(gsquare > 0, values, math.pi / (screen_omega * screen_omega))
    return values * (-mixing / float(NG) ** 3)


def kernel_axes():
    band = lax.axis_index("band")
    return band % 4, band // 4, lax.axis_index("plane")


def send(source, target, send_sem, recv_sem, device):
    return pltpu.make_async_remote_copy(
        src_ref=source, dst_ref=target, send_sem=send_sem, recv_sem=recv_sem,
        device_id=device, device_id_type=MESH,
    )


def spread(psi_hbm, half_hbm, send_sem, recv_sem):
    x, zh, me = kernel_axes()

    def half(i):
        return send(
            psi_hbm.at[pl.ds(LINES * i + HALF, HALF), 0], half_hbm.at[i, pl.ds(0, HALF)],
            send_sem.at[i], recv_sem.at[i], (zh * 4 + 3 - x, me),
        )

    @pl.when(zh == 0)
    def _():
        barrier = pltpu.get_barrier_semaphore()
        pl.semaphore_signal(barrier, inc=1, device_id=(zh * 4 + 3 - x, me), device_id_type=MESH)
        pl.semaphore_wait(barrier, 1)

        @pl.when(x < 2)
        def _():
            for i in range(THICK):
                half(i).start()
            for i in range(THICK):
                half(i).wait_send()

        @pl.when(x >= 2)
        def _():
            for i in range(THICK):
                half(i).wait_recv()


def body(
    psi_hbm, half_hbm, tab_hbm, out,
    psi, tab, src, psi_y, src_y, kern, s_out, r_in, g_out, h_in,
    load_sem, own_sem, zs, zr, xs, xr, fs, fr, bs, br,
):
    x, zh, me = kernel_axes()
    band = zh * 4 + x

    def at_x(d):
        return (zh * 4 + (x + d) % 4, me)

    def at_z(d):
        return (((zh + d) % 4) * 4 + x, me)

    def share_of(d):
        y, z, c = me // 4, (me // 2) % 2, me % 2
        return ((y + d // 4) % 4) * 4 + ((z + (d // 2) % 2) % 2) * 2 + (c + d % 2) % 2

    def at_plane(d):
        return (band, share_of(d))

    barrier = pltpu.get_barrier_semaphore()
    peers = [at_x(d) for d in (1, 2, 3)] + [at_z(d) for d in (1, 2, 3)]
    peers += [at_plane(d) for d in range(1, SHARES)]
    for peer in peers:
        pl.semaphore_signal(barrier, inc=1, device_id=peer, device_id_type=MESH)

    load_psi = pltpu.make_async_copy(psi_hbm.at[:, 0], psi, load_sem.at[0])
    load_psi.start()
    load_tab = pltpu.make_async_copy(tab_hbm, tab, load_sem.at[1])
    load_tab.start()

    own_source, own_half = ((x + 1) // 2) % 2, x // 2

    def piece(i):
        return src.at[own_source, own_half, i, pl.ds(0, HALF)]

    def own_from_psi(i):
        return pltpu.make_async_copy(psi_hbm.at[pl.ds(LINES * i, HALF), 0], piece(i), own_sem.at[i])

    def own_from_half(i):
        return pltpu.make_async_copy(half_hbm.at[i, pl.ds(0, HALF)], piece(i), own_sem.at[i])

    @pl.when(zh == 0)
    def _():
        @pl.when(x < 2)
        def _():
            for i in range(THICK):
                own_from_psi(i).start()

        @pl.when(x >= 2)
        def _():
            for i in range(THICK):
                own_from_half(i).start()

    lane = lax.broadcasted_iota(jnp.int32, (HALF // 7, 128), 1)

    def to_rows(rows, at):
        flat = [rows(b) for b in range(7)]
        for a in range(8):
            if a == 0:
                value = flat[0]
            else:
                below = flat[a] if a < 7 else jnp.zeros_like(flat[0])
                value = pltpu.roll(jnp.where(lane < 128 - 16 * a, below, flat[a - 1]), 16 * a, 1)
            at(a, value)

    def along_z(d, i):
        return send(piece(i), piece(i), zs.at[d - 1, i], zr.at[i], at_z(d))

    def along_x(d, i):
        return send(piece(i), piece(i), xs.at[d - 1, i], xr.at[i], at_x(d))

    def from_origin(act):
        @pl.when(zh == 0)
        def _():
            for i in (0, 2, 4, 6):
                act(along_z(2, i))
            for i in (1, 3, 5):
                for d in (3, 1):
                    act(along_z(d, i))

    def passed_on(i, act):
        relay = 2 if i % 2 == 0 else 3 if i == 3 else 1

        @pl.when(zh == relay)
        def _():
            for d in (1, 3) if relay == 2 else (relay,):
                act(along_z(d, i))

    @pl.when(zh == 0)
    def _():
        for i in range(THICK):
            own_from_psi(i).wait()
        pl.semaphore_wait(barrier, len(peers))

    from_origin(lambda copy: copy.start())

    for buffer in (r_in, h_in):
        for share in range(SHARES):
            rows = slice(BLOCK * share + USED, BLOCK * (share + 1))
            buffer[rows, :] = jnp.zeros((BLOCK - USED, 128), f32)
    load_psi.wait()
    for i in range(THICK):
        for h in range(2):
            def put(a, value, i=i, h=h):
                psi_y[pl.ds(NG * i + 56 * h + a, 7, stride=8), :] = value

            to_rows(lambda b, i=i, h=h: psi[pl.ds(LINES * i + HALF * h + b, 7, stride=7), :], put)
    for k in range(THICK):
        kern[k] = kernel_tile(THICK * me + k, (128, 128))
    load_tab.wait()

    @pl.when(zh != 0)
    def _():
        pl.semaphore_wait(barrier, len(peers))

    def block(buffer, share, start, count):
        return buffer.at[pl.ds(BLOCK * share + start, count)]

    def exchange(source, target, send_sem, recv_sem, d, i):
        return send(
            block(source, share_of(d), ROWS * i, ROWS), block(target, me, ROWS * i, ROWS),
            send_sem, recv_sem, at_plane(d),
        )

    def keep(source, target):
        rows = pl.ds(pl.multiple_of(BLOCK * me, 8), BLOCK)
        target[rows, :] = source[rows, :]

    def forward(i):
        rows = slice(NG * i, NG * (i + 1))
        for j in range(2):
            for h in range(2):
                def put(a, value, j=j, h=h):
                    src_y[j, pl.ds(NG * i + 56 * h + a, 7, stride=8), :] = value

                to_rows(lambda b, j=j, h=h: src[j, h, i, pl.ds(b, 7, stride=7), :], put)
        field = psi_y[rows, :]
        density = jnp.concatenate([field * src_y[0, rows, :], field * src_y[1, rows, :]], axis=1)
        values = from_right(density, tab[0], tab[1])
        values = jnp.concatenate([values[:, 0:128], values[:, 128:256]], axis=0)
        values = from_left(tab[2, :, 0 : 2 * NG], tab[3, :, 0 : 2 * NG], values)
        for share in range(SHARES):
            start = BLOCK * share + ROWS * i
            s_out[start : start + ROWS, :] = values[16 * share : 16 * share + ROWS, :]

    def pass_on(i):
        @pl.when(zh != 0)
        def _():
            along_z(1, i).wait_recv()

        passed_on(i, lambda copy: copy.start())
        for d in (1, 3, 2):
            along_x(d, i).start()

    def take(i):
        gone = s_out.at[pl.ds(0, 3 * HALF)]
        send(gone, gone, xs.at[0, i], xr.at[i], at_x(1)).wait_recv()
        forward(i)
        for d in ORDER:
            exchange(s_out, r_in, fs, fr, d, i).start()

    def in_order(steps):
        for step in steps:
            (pass_on if step < 0 else take)(abs(step) - 1)

    @pl.when(zh == 2)
    def _():
        in_order(EVEN_FIRST)

    @pl.when(zh != 2)
    def _():
        in_order(ODD_FIRST)

    keep(s_out, r_in)
    whole = pl.ds(0, (SHARES - 1) * USED)
    send(s_out.at[whole], r_in.at[whole], fs, fr, at_plane(1)).wait_recv()

    def first_part(waves):
        columns = []
        for k in waves:
            columns.append(jnp.concatenate(
                [r_in[pl.ds(k, 128, stride=ROWS), :], r_in[pl.ds(THICK + k, 128, stride=ROWS), :]], axis=0))
        spectrum = from_left(tab[4], tab[5], jnp.concatenate(columns, axis=1))
        factor = jnp.concatenate([kern[k] for k in waves], axis=1)
        return spectrum * jnp.concatenate([factor, factor], axis=0)

    def second_part(waves, spectrum):
        result = from_left(tab[6], tab[7], spectrum)
        for place, k in enumerate(waves):
            lanes = slice(128 * place, 128 * (place + 1))
            g_out[pl.ds(k, 128, stride=ROWS), :] = result[0:128, lanes]
            g_out[pl.ds(THICK + k, 128, stride=ROWS), :] = result[128:256, lanes]

    groups = ((0, 1), (2, 3), (4, 5), (6,))
    held = [first_part(waves) for waves in groups]
    for waves, spectrum in zip(groups, held):
        second_part(waves, spectrum)

    for i in reversed(range(THICK)):
        for d in ORDER:
            exchange(g_out, h_in, bs, br.at[i], d, i).start()
    keep(g_out, h_in)

    def result(i):
        rows = pl.ds(LINES * i, LINES)
        return pltpu.make_async_copy(psi.at[rows], out.at[rows, 0], own_sem.at[i])

    out_lane = lax.broadcasted_iota(jnp.int32, (NG // 8, 128), 1)

    def back(i):
        columns = [h_in[BLOCK * q + ROWS * i : BLOCK * q + ROWS * i + 16, :] for q in range(SHARES)]
        values = from_left(tab[8, 0 : 2 * NG], tab[9, 0 : 2 * NG], jnp.concatenate(columns, axis=0))
        both = jnp.concatenate([values[0:NG], values[NG : 2 * NG]], axis=1)
        potential = from_right(both, tab[10], tab[11])
        rows = slice(NG * i, NG * (i + 1))
        psi_y[rows, :] = potential[:, 0:128] * src_y[0, rows, :] + potential[:, 128:256] * src_y[1, rows, :]
        turned = []
        for a in range(8):
            value = psi_y[pl.ds(NG * i + a, NG // 8, stride=8), :]
            turned.append(pltpu.roll(value, 128 - 16 * a, 1) if a else value)
        for b in range(7):
            value = jnp.where(out_lane < NG - 16 * b, turned[b], turned[b + 1])
            out[pl.ds(LINES * i + b, NG // 8, stride=7), 0, :] = value

    for i in reversed(range(THICK)):
        rows = pl.ds(0, (SHARES - 1) * ROWS)
        send(g_out.at[rows], h_in.at[rows], bs, br.at[i], at_plane(1)).wait_recv()
        back(i)

    from_origin(lambda copy: copy.wait_send())
    for i in range(THICK):
        passed_on(i, lambda copy: copy.wait_send())
        for d in (1, 3, 2):
            along_x(d, i).wait_send()
    send(s_out.at[whole], r_in.at[whole], fs, fr, at_plane(1)).wait_send()
    send(g_out.at[whole], h_in.at[whole], bs, br.at[0], at_plane(1)).wait_send()


def on_device(orbitals):
    table = jnp.asarray(tables())
    field = orbitals.reshape(THICK * LINES, 1, 128)
    dma = pltpu.SemaphoreType.DMA
    vmem = pltpu.VMEM
    anywhere = pl.BlockSpec(memory_space=pl.ANY)
    half = pl.pallas_call(
        spread,
        out_shape=jax.ShapeDtypeStruct((THICK, 56, 128), f32),
        in_specs=[anywhere],
        out_specs=anywhere,
        scratch_shapes=[dma((THICK,)), dma((THICK,))],
        compiler_params=pltpu.CompilerParams(collective_id=1, has_side_effects=True),
    )(field)
    exchanged = vmem((SHARES * BLOCK, 128), f32)
    total = pl.pallas_call(
        body,
        out_shape=pltpu.VMEM((THICK * LINES, 1, 128), f32),
        in_specs=[anywhere] * 3,
        out_specs=pl.BlockSpec(memory_space=vmem),
        scratch_shapes=[
            vmem((THICK * LINES, 128), f32),
            vmem((12, 256, 256), bf16),
            vmem((2, 2, THICK, 56, 128), f32),
            vmem((THICK * NG, 128), f32),
            vmem((2, THICK * NG, 128), f32),
            vmem((THICK, 128, 128), f32),
            exchanged, exchanged, exchanged, exchanged,
            dma((2,)), dma((THICK,)), dma((3, THICK)), dma((THICK,)), dma((3, THICK)), dma((THICK,)),
            dma, dma, dma, dma((THICK,)),
        ],
        compiler_params=pltpu.CompilerParams(collective_id=0, has_side_effects=True),
    )(field, half, table)
    return total.reshape(orbitals.shape)


def solution(mesh):
    spec = P("band", "plane", None)
    return jax.shard_map(on_device, mesh=mesh, in_specs=(spec,), out_specs=spec, check_vma=False)
```

```python
import math

import jax
import jax.numpy as jnp
import ml_dtypes
import numpy as np
from jax import lax
from jax.experimental import pallas as pl
from jax.experimental.pallas import tpu as pltpu
from jax.sharding import PartitionSpec as P

MESH = pl.DeviceIdType.MESH
NG = 112
FLAT = NG * NG
LINES = FLAT // 128
HALF = LINES // 2
EVEN_FIRST = (-1, -3, -5, 1, 3, -2, 5, -4, -6, 2, -7, 4, 6, 7)
ODD_FIRST = (-2, -4, -6, -1, 2, -7, -3, 4, -5, 6, 1, 7, 3, 5)
SHARES = 16
THICK = NG // SHARES
ROWS = 2 * THICK
BLOCK = 112
SENT = ROWS - 1
USED = THICK * ROWS
ORDER = (10, 11, 8, 9, 6, 14, 7, 13, 2, 3, 4, 12, 5, 15, 1)
screen_omega = 0.106
cell_length = 46.93
mixing = 0.25
f32, bf16 = jnp.float32, jnp.bfloat16


def tables():
    index = np.arange(NG)
    angle = (index[:, None] * index[None, :] % NG) * (2.0 * math.pi / NG)
    cos, sin = np.cos(angle), np.sin(angle)
    re, im = slice(0, NG), slice(128, 128 + NG)
    last = np.zeros((256, 256))
    last[re, re], last[im, re] = cos, sin
    last[re, im], last[im, im] = -sin, cos
    last_back = np.zeros((256, 256))
    last_back[re, re], last_back[im, re] = cos, -sin
    last_back[re, im], last_back[im, im] = sin, cos
    second = np.zeros((256, 256))
    second_back = np.zeros((256, 256))
    for share in range(SHARES):
        for part in range(2):
            for k in range(THICK):
                row, wave = 16 * share + THICK * part + k, THICK * share + k
                if part == 0:
                    second[row, 0:NG], second[row, NG : 2 * NG] = cos[wave], sin[wave]
                    second_back[0:NG, row], second_back[NG : 2 * NG, row] = cos[wave], sin[wave]
                else:
                    second[row, 0:NG], second[row, NG : 2 * NG] = -sin[wave], cos[wave]
                    second_back[0:NG, row], second_back[NG : 2 * NG, row] = -sin[wave], cos[wave]
    place = 8 * (index // THICK) + index % THICK
    first = np.zeros((256, 256))
    first_back = np.zeros((256, 256))
    first[re, place], first[re, 128 + place] = cos, sin
    first[im, place], first[im, 128 + place] = -sin, cos
    first_back[place, re], first_back[place, im] = cos, -sin
    first_back[128 + place, re], first_back[128 + place, im] = sin, cos
    both = []
    for table in (last, second, first, first_back, second_back, last_back):
        high = table.astype(ml_dtypes.bfloat16)
        both += [high, (table - high.astype(np.float64)).astype(ml_dtypes.bfloat16)]
    return np.stack(both)


def split(values):
    high = values.astype(bf16)
    return high, (values - high.astype(f32)).astype(bf16)


def dot(a, b):
    return jnp.dot(a, b, preferred_element_type=f32)


def from_left(high, low, values):
    big, small = split(values)
    return dot(high, big) + dot(high, small) + dot(low, big)


def from_right(values, high, low):
    big, small = split(values)
    return dot(big, high) + dot(small, high) + dot(big, low)


def kernel_tile(k_second, shape):
    def wave(index):
        return jnp.where(2 * index < NG, index, index - NG).astype(f32)

    first = wave(lax.broadcasted_iota(jnp.int32, shape, 0))
    last = wave(lax.broadcasted_iota(jnp.int32, shape, 1))
    second = wave(jnp.full(shape, k_second, jnp.int32))
    gsquare = (first * first + second * second + last * last) * (2.0 * math.pi / cell_length) ** 2
    safe = jnp.where(gsquare > 0, gsquare, 1.0)
    values = 4.0 * math.pi / safe * (1.0 - jnp.exp(-safe / (4.0 * screen_omega * screen_omega)))
    values = jnp.where(gsquare > 0, values, math.pi / (screen_omega * screen_omega))
    return values * (-mixing / float(NG) ** 3)


def kernel_axes():
    band = lax.axis_index("band")
    return band % 4, band // 4, lax.axis_index("plane")


def send(source, target, send_sem, recv_sem, device):
    return pltpu.make_async_remote_copy(
        src_ref=source, dst_ref=target, send_sem=send_sem, recv_sem=recv_sem,
        device_id=device, device_id_type=MESH,
    )


def spread(psi_hbm, half_hbm, send_sem, recv_sem):
    x, zh, me = kernel_axes()

    def half(i):
        return send(
            psi_hbm.at[pl.ds(LINES * i + HALF, HALF), 0], half_hbm.at[i, pl.ds(0, HALF)],
            send_sem.at[i], recv_sem.at[i], (zh * 4 + 3 - x, me),
        )

    @pl.when(zh == 0)
    def _():
        barrier = pltpu.get_barrier_semaphore()
        pl.semaphore_signal(barrier, inc=1, device_id=(zh * 4 + 3 - x, me), device_id_type=MESH)
        pl.semaphore_wait(barrier, 1)

        @pl.when(x < 2)
        def _():
            for i in range(THICK):
                half(i).start()
            for i in range(THICK):
                half(i).wait_send()

        @pl.when(x >= 2)
        def _():
            for i in range(THICK):
                half(i).wait_recv()


def body(
    psi_hbm, half_hbm, tab_hbm, out,
    psi, tab, src, psi_y, src_y, kern, s_out, r_in, g_out, h_in,
    load_sem, own_sem, zs, zr, xs, xr, fs, fr, bs, br,
):
    x, zh, me = kernel_axes()
    band = zh * 4 + x

    def at_x(d):
        return (zh * 4 + (x + d) % 4, me)

    def at_z(d):
        return (((zh + d) % 4) * 4 + x, me)

    def share_of(d):
        y, z, c = me // 4, (me // 2) % 2, me % 2
        return ((y + d // 4) % 4) * 4 + ((z + (d // 2) % 2) % 2) * 2 + (c + d % 2) % 2

    def at_plane(d):
        return (band, share_of(d))

    barrier = pltpu.get_barrier_semaphore()
    peers = [at_x(d) for d in (1, 2, 3)] + [at_z(d) for d in (1, 2, 3)]
    peers += [at_plane(d) for d in range(1, SHARES)]
    for peer in peers:
        pl.semaphore_signal(barrier, inc=1, device_id=peer, device_id_type=MESH)

    load_psi = pltpu.make_async_copy(psi_hbm.at[:, 0], psi, load_sem.at[0])
    load_psi.start()
    load_tab = pltpu.make_async_copy(tab_hbm, tab, load_sem.at[1])
    load_tab.start()

    own_source, own_half = ((x + 1) // 2) % 2, x // 2

    def piece(i):
        return src.at[own_source, own_half, i, pl.ds(0, HALF)]

    def own_from_psi(i):
        return pltpu.make_async_copy(psi_hbm.at[pl.ds(LINES * i, HALF), 0], piece(i), own_sem.at[i])

    def own_from_half(i):
        return pltpu.make_async_copy(half_hbm.at[i, pl.ds(0, HALF)], piece(i), own_sem.at[i])

    @pl.when(zh == 0)
    def _():
        @pl.when(x < 2)
        def _():
            for i in range(THICK):
                own_from_psi(i).start()

        @pl.when(x >= 2)
        def _():
            for i in range(THICK):
                own_from_half(i).start()

    lane = lax.broadcasted_iota(jnp.int32, (HALF // 7, 128), 1)

    def to_rows(rows, at):
        flat = [rows(b) for b in range(7)]
        for a in range(8):
            if a == 0:
                value = flat[0]
            else:
                below = flat[a] if a < 7 else jnp.zeros_like(flat[0])
                value = pltpu.roll(jnp.where(lane < 128 - 16 * a, below, flat[a - 1]), 16 * a, 1)
            at(a, value)

    def along_z(d, i):
        return send(piece(i), piece(i), zs.at[d - 1, i], zr.at[i], at_z(d))

    def along_x(d, i):
        return send(piece(i), piece(i), xs.at[d - 1, i], xr.at[i], at_x(d))

    def from_origin(act):
        @pl.when(zh == 0)
        def _():
            for i in (0, 2, 4):
                act(along_z(2, i))
            for i in (1, 3, 5, 6):
                for d in (3, 1):
                    act(along_z(d, i))

    def passed_on(i, act):
        relay = (2, 1, 2, 3, 2, 1, 3)[i]

        @pl.when(zh == relay)
        def _():
            for d in (1, 3) if relay == 2 else (relay,):
                act(along_z(d, i))

    @pl.when(zh == 0)
    def _():
        for i in range(THICK):
            own_from_psi(i).wait()
        pl.semaphore_wait(barrier, len(peers))

    from_origin(lambda copy: copy.start())

    for buffer in (r_in, h_in):
        for share in range(SHARES):
            rows = slice(BLOCK * share + USED, BLOCK * (share + 1))
            buffer[rows, :] = jnp.zeros((BLOCK - USED, 128), f32)
    load_psi.wait()
    for i in range(THICK):
        for h in range(2):
            def put(a, value, i=i, h=h):
                psi_y[pl.ds(NG * i + 56 * h + a, 7, stride=8), :] = value

            to_rows(lambda b, i=i, h=h: psi[pl.ds(LINES * i + HALF * h + b, 7, stride=7), :], put)
    for k in range(THICK):
        kern[k] = kernel_tile(THICK * me + k, (128, 128))
    load_tab.wait()

    @pl.when(zh != 0)
    def _():
        pl.semaphore_wait(barrier, len(peers))

    def block(buffer, share, start, count):
        return buffer.at[pl.ds(BLOCK * share + start, count)]

    def exchange(source, target, send_sem, recv_sem, d, i, rows=ROWS):
        return send(
            block(source, share_of(d), ROWS * i, rows), block(target, me, ROWS * i, rows),
            send_sem, recv_sem, at_plane(d),
        )

    def keep(source, target):
        rows = pl.ds(pl.multiple_of(BLOCK * me, 8), BLOCK)
        target[rows, :] = source[rows, :]

    def of_all(i, row):
        return pl.ds(ROWS * i + row, SHARES, stride=BLOCK)

    def tucked(row, last, g):
        lanes = lax.broadcasted_iota(jnp.int32, row.shape, 1)
        return jnp.where(lanes < NG, row, pltpu.roll(last, NG - 16 * g, 1))

    def untucked(row):
        last = pltpu.roll(row(0), 16, 1)
        lanes = lax.broadcasted_iota(jnp.int32, last.shape, 1)
        for g in range(1, 7):
            last = jnp.where(lanes < 16 * g, last, pltpu.roll(row(g), 16 + 16 * g, 1))
        return last

    def forward(i):
        rows = slice(NG * i, NG * (i + 1))
        for j in range(2):
            for h in range(2):
                def put(a, value, j=j, h=h):
                    src_y[j, pl.ds(NG * i + 56 * h + a, 7, stride=8), :] = value

                to_rows(lambda b, j=j, h=h: src[j, h, i, pl.ds(b, 7, stride=7), :], put)
        field = psi_y[rows, :]
        density = jnp.concatenate([field * src_y[0, rows, :], field * src_y[1, rows, :]], axis=1)
        values = from_right(density, tab[0], tab[1])
        values = jnp.concatenate([values[:, 0:128], values[:, 128:256]], axis=0)
        values = from_left(tab[2, :, 0 : 2 * NG], tab[3, :, 0 : 2 * NG], values)
        for share in range(SHARES):
            start = BLOCK * share + ROWS * i
            s_out[start : start + ROWS, :] = values[16 * share : 16 * share + ROWS, :]

    def pass_on(i):
        @pl.when(zh != 0)
        def _():
            along_z(1, i).wait_recv()

        passed_on(i, lambda copy: copy.start())
        for d in (1, 3, 2):
            along_x(d, i).start()

    def take(i):
        gone = s_out.at[pl.ds(0, 3 * HALF)]
        send(gone, gone, xs.at[0, i], xr.at[i], at_x(1)).wait_recv()
        forward(i)
        for d in ORDER:
            exchange(s_out, r_in, fs, fr, d, i).start()

    def in_order(steps):
        for step in steps:
            (pass_on if step < 0 else take)(abs(step) - 1)

    @pl.when(zh == 2)
    def _():
        in_order(EVEN_FIRST)

    @pl.when(zh != 2)
    def _():
        in_order(ODD_FIRST)

    keep(s_out, r_in)
    whole = pl.ds(0, (SHARES - 1) * USED)
    packed = pl.ds(0, (SHARES - 1) * THICK * SENT)
    send(s_out.at[whole], r_in.at[whole], fs, fr, at_plane(1)).wait_recv()

    def first_part(waves):
        columns = []
        for k in waves:
            def row(t):
                return r_in[pl.ds(t, 128, stride=ROWS), :]

            columns.append(jnp.concatenate([row(k), row(THICK + k)], axis=0))
        spectrum = from_left(tab[4], tab[5], jnp.concatenate(columns, axis=1))
        factor = jnp.concatenate([kern[k] for k in waves], axis=1)
        return spectrum * jnp.concatenate([factor, factor], axis=0)

    def second_part(waves, spectrum, last):
        result = from_left(tab[6], tab[7], spectrum)
        if last is None:
            last = result[128:256]
        for place, k in enumerate(waves):
            lanes = slice(128 * place, 128 * (place + 1))
            g_out[pl.ds(k, 128, stride=ROWS), :] = tucked(result[0:128, lanes], last, k)
            g_out[pl.ds(THICK + k, 128, stride=ROWS), :] = result[128:256, lanes]
        return last

    groups = ((0, 1), (2, 3), (4, 5), (6,))
    held = [first_part(waves) for waves in groups]
    last = None
    for waves, spectrum in zip(groups[::-1], held[::-1]):
        last = second_part(waves, spectrum, last)

    for i in reversed(range(THICK)):
        for d in ORDER:
            exchange(g_out, h_in, bs, br.at[i], d, i, SENT).start()
    keep(g_out, h_in)

    def result(i):
        rows = pl.ds(LINES * i, LINES)
        return pltpu.make_async_copy(psi.at[rows], out.at[rows, 0], own_sem.at[i])

    out_lane = lax.broadcasted_iota(jnp.int32, (NG // 8, 128), 1)

    def back(i):
        h_in[of_all(i, SENT), :] = untucked(lambda g: h_in[of_all(i, g), :])
        columns = [h_in[BLOCK * q + ROWS * i : BLOCK * q + ROWS * i + 16, :] for q in range(SHARES)]
        values = from_left(tab[8, 0 : 2 * NG], tab[9, 0 : 2 * NG], jnp.concatenate(columns, axis=0))
        both = jnp.concatenate([values[0:NG], values[NG : 2 * NG]], axis=1)
        potential = from_right(both, tab[10], tab[11])
        rows = slice(NG * i, NG * (i + 1))
        psi_y[rows, :] = potential[:, 0:128] * src_y[0, rows, :] + potential[:, 128:256] * src_y[1, rows, :]
        turned = []
        for a in range(8):
            value = psi_y[pl.ds(NG * i + a, NG // 8, stride=8), :]
            turned.append(pltpu.roll(value, 128 - 16 * a, 1) if a else value)
        for b in range(7):
            value = jnp.where(out_lane < NG - 16 * b, turned[b], turned[b + 1])
            out[pl.ds(LINES * i + b, NG // 8, stride=7), 0, :] = value

    for i in reversed(range(THICK)):
        rows = pl.ds(0, (SHARES - 1) * SENT)
        send(g_out.at[rows], h_in.at[rows], bs, br.at[i], at_plane(1)).wait_recv()
        back(i)

    from_origin(lambda copy: copy.wait_send())
    for i in range(THICK):
        passed_on(i, lambda copy: copy.wait_send())
        for d in (1, 3, 2):
            along_x(d, i).wait_send()
    send(s_out.at[whole], r_in.at[whole], fs, fr, at_plane(1)).wait_send()
    send(g_out.at[packed], h_in.at[packed], bs, br.at[0], at_plane(1)).wait_send()


def on_device(orbitals):
    table = jnp.asarray(tables())
    field = orbitals.reshape(THICK * LINES, 1, 128)
    dma = pltpu.SemaphoreType.DMA
    vmem = pltpu.VMEM
    anywhere = pl.BlockSpec(memory_space=pl.ANY)
    half = pl.pallas_call(
        spread,
        out_shape=jax.ShapeDtypeStruct((THICK, 56, 128), f32),
        in_specs=[anywhere],
        out_specs=anywhere,
        scratch_shapes=[dma((THICK,)), dma((THICK,))],
        compiler_params=pltpu.CompilerParams(collective_id=1, has_side_effects=True),
    )(field)
    exchanged = vmem((SHARES * BLOCK, 128), f32)
    total = pl.pallas_call(
        body,
        out_shape=pltpu.VMEM((THICK * LINES, 1, 128), f32),
        in_specs=[anywhere] * 3,
        out_specs=pl.BlockSpec(memory_space=vmem),
        scratch_shapes=[
            vmem((THICK * LINES, 128), f32),
            vmem((12, 256, 256), bf16),
            vmem((2, 2, THICK, 56, 128), f32),
            vmem((THICK * NG, 128), f32),
            vmem((2, THICK * NG, 128), f32),
            vmem((THICK, 128, 128), f32),
            exchanged, exchanged, exchanged, exchanged,
            dma((2,)), dma((THICK,)), dma((3, THICK)), dma((THICK,)), dma((3, THICK)), dma((THICK,)),
            dma, dma, dma, dma((THICK,)),
        ],
        compiler_params=pltpu.CompilerParams(collective_id=0, has_side_effects=True),
    )(field, half, table)
    return total.reshape(orbitals.shape)


def solution(mesh):
    spec = P("band", "plane", None)
    return jax.shard_map(on_device, mesh=mesh, in_specs=(spec,), out_specs=spec, check_vma=False)
```

```python
import math

import jax
import jax.numpy as jnp
import ml_dtypes
import numpy as np
from jax import lax
from jax.experimental import pallas as pl
from jax.experimental.pallas import tpu as pltpu
from jax.sharding import PartitionSpec as P

MESH = pl.DeviceIdType.MESH
NG = 112
FLAT = NG * NG
LINES = FLAT // 128
HALF = LINES // 2
EVEN_FIRST = (-1, -3, -5, 1, 3, -2, 5, -4, -6, 2, -7, 4, 6, 7)
ODD_FIRST = (-2, -4, -6, -1, 2, -7, -3, 4, -5, 6, 1, 7, 3, 5)
SHARES = 16
THICK = NG // SHARES
ROWS = 2 * THICK
BLOCK = 112
SENT = ROWS - 1
USED = THICK * ROWS
ORDER = (10, 11, 8, 9, 6, 14, 7, 13, 2, 3, 4, 12, 5, 15, 1)
screen_omega = 0.106
cell_length = 46.93
mixing = 0.25
f32, bf16 = jnp.float32, jnp.bfloat16


def tables():
    index = np.arange(NG)
    angle = (index[:, None] * index[None, :] % NG) * (2.0 * math.pi / NG)
    cos, sin = np.cos(angle), np.sin(angle)
    re, im = slice(0, NG), slice(128, 128 + NG)
    last = np.zeros((256, 256))
    last[re, re], last[im, re] = cos, sin
    last[re, im], last[im, im] = -sin, cos
    last_back = np.zeros((256, 256))
    last_back[re, re], last_back[im, re] = cos, -sin
    last_back[re, im], last_back[im, im] = sin, cos
    second = np.zeros((256, 256))
    second_back = np.zeros((256, 256))
    for share in range(SHARES):
        for part in range(2):
            for k in range(THICK):
                row, wave = 16 * share + THICK * part + k, THICK * share + k
                if part == 0:
                    second[row, 0:NG], second[row, NG : 2 * NG] = cos[wave], sin[wave]
                    second_back[0:NG, row], second_back[NG : 2 * NG, row] = cos[wave], sin[wave]
                else:
                    second[row, 0:NG], second[row, NG : 2 * NG] = -sin[wave], cos[wave]
                    second_back[0:NG, row], second_back[NG : 2 * NG, row] = -sin[wave], cos[wave]
    place = 8 * (index // THICK) + index % THICK
    first = np.zeros((256, 256))
    first_back = np.zeros((256, 256))
    first[re, place], first[re, 128 + place] = cos, sin
    tail = slice(NG, 2 * NG)
    first[tail, place], first[tail, 128 + place] = -sin, cos
    first_back[place, re], first_back[place, tail] = cos, -sin
    first_back[128 + place, re], first_back[128 + place, tail] = sin, cos
    both = []
    for table in (last, second, first, first_back, second_back, last_back):
        high = table.astype(ml_dtypes.bfloat16)
        both += [high, (table - high.astype(np.float64)).astype(ml_dtypes.bfloat16)]
    return np.stack(both)


def split(values):
    high = values.astype(bf16)
    return high, (values - high.astype(f32)).astype(bf16)


def dot(a, b):
    return jnp.dot(a, b, preferred_element_type=f32)


def from_left(high, low, values):
    big, small = split(values)
    return dot(high, big) + dot(high, small) + dot(low, big)


def from_right(values, high, low):
    big, small = split(values)
    return dot(big, high) + dot(small, high) + dot(big, low)


def kernel_tile(k_second, shape):
    def wave(index):
        return jnp.where(2 * index < NG, index, index - NG).astype(f32)

    first = wave(lax.broadcasted_iota(jnp.int32, shape, 0))
    last = wave(lax.broadcasted_iota(jnp.int32, shape, 1))
    second = wave(jnp.full(shape, k_second, jnp.int32))
    gsquare = (first * first + second * second + last * last) * (2.0 * math.pi / cell_length) ** 2
    safe = jnp.where(gsquare > 0, gsquare, 1.0)
    values = 4.0 * math.pi / safe * (1.0 - jnp.exp(-safe / (4.0 * screen_omega * screen_omega)))
    values = jnp.where(gsquare > 0, values, math.pi / (screen_omega * screen_omega))
    return values * (-mixing / float(NG) ** 3)


def kernel_axes():
    band = lax.axis_index("band")
    return band % 4, band // 4, lax.axis_index("plane")


def send(source, target, send_sem, recv_sem, device):
    return pltpu.make_async_remote_copy(
        src_ref=source, dst_ref=target, send_sem=send_sem, recv_sem=recv_sem,
        device_id=device, device_id_type=MESH,
    )


def spread(psi_hbm, half_hbm, send_sem, recv_sem):
    x, zh, me = kernel_axes()

    def half(i):
        return send(
            psi_hbm.at[pl.ds(LINES * i + HALF, HALF), 0], half_hbm.at[i, pl.ds(0, HALF)],
            send_sem.at[i], recv_sem.at[i], (zh * 4 + 3 - x, me),
        )

    @pl.when(zh == 0)
    def _():
        barrier = pltpu.get_barrier_semaphore()
        pl.semaphore_signal(barrier, inc=1, device_id=(zh * 4 + 3 - x, me), device_id_type=MESH)
        pl.semaphore_wait(barrier, 1)

        @pl.when(x < 2)
        def _():
            for i in range(THICK):
                half(i).start()
            for i in range(THICK):
                half(i).wait_send()

        @pl.when(x >= 2)
        def _():
            for i in range(THICK):
                half(i).wait_recv()


def body(
    psi_hbm, half_hbm, tab_hbm, out,
    psi, tab, src, psi_y, src_y, kern, s_out, r_in, g_out, h_in,
    load_sem, own_sem, zs, zr, xs, xr, fs, fr, bs, br,
):
    x, zh, me = kernel_axes()
    band = zh * 4 + x

    def at_x(d):
        return (zh * 4 + (x + d) % 4, me)

    def at_z(d):
        return (((zh + d) % 4) * 4 + x, me)

    def share_of(d):
        y, z, c = me // 4, (me // 2) % 2, me % 2
        return ((y + d // 4) % 4) * 4 + ((z + (d // 2) % 2) % 2) * 2 + (c + d % 2) % 2

    def at_plane(d):
        return (band, share_of(d))

    barrier = pltpu.get_barrier_semaphore()
    peers = [at_x(d) for d in (1, 2, 3)] + [at_z(d) for d in (1, 2, 3)]
    peers += [at_plane(d) for d in range(1, SHARES)]
    for peer in peers:
        pl.semaphore_signal(barrier, inc=1, device_id=peer, device_id_type=MESH)

    load_psi = pltpu.make_async_copy(psi_hbm.at[:, 0], psi, load_sem.at[0])
    load_psi.start()
    load_tab = pltpu.make_async_copy(tab_hbm, tab, load_sem.at[1])
    load_tab.start()

    own_source, own_half = ((x + 1) // 2) % 2, x // 2

    def piece(i):
        return src.at[own_source, own_half, i, pl.ds(0, HALF)]

    def own_from_psi(i):
        return pltpu.make_async_copy(psi_hbm.at[pl.ds(LINES * i, HALF), 0], piece(i), own_sem.at[i])

    def own_from_half(i):
        return pltpu.make_async_copy(half_hbm.at[i, pl.ds(0, HALF)], piece(i), own_sem.at[i])

    @pl.when(zh == 0)
    def _():
        @pl.when(x < 2)
        def _():
            for i in range(THICK):
                own_from_psi(i).start()

        @pl.when(x >= 2)
        def _():
            for i in range(THICK):
                own_from_half(i).start()

    lane = lax.broadcasted_iota(jnp.int32, (HALF // 7, 128), 1)

    def to_rows(rows, at):
        flat = [rows(b) for b in range(7)]
        for a in range(8):
            if a == 0:
                value = flat[0]
            else:
                below = flat[a] if a < 7 else jnp.zeros_like(flat[0])
                value = pltpu.roll(jnp.where(lane < 128 - 16 * a, below, flat[a - 1]), 16 * a, 1)
            at(a, value)

    def along_z(d, i):
        return send(piece(i), piece(i), zs.at[d - 1, i], zr.at[i], at_z(d))

    def along_x(d, i):
        return send(piece(i), piece(i), xs.at[d - 1, i], xr.at[i], at_x(d))

    def from_origin(act):
        @pl.when(zh == 0)
        def _():
            for i in (0, 2, 4):
                act(along_z(2, i))
            for i in (1, 3, 5, 6):
                for d in (3, 1):
                    act(along_z(d, i))

    def passed_on(i, act):
        relay = (2, 1, 2, 3, 2, 1, 3)[i]

        @pl.when(zh == relay)
        def _():
            for d in (1, 3) if relay == 2 else (relay,):
                act(along_z(d, i))

    @pl.when(zh == 0)
    def _():
        for i in range(THICK):
            own_from_psi(i).wait()
        pl.semaphore_wait(barrier, len(peers))

    from_origin(lambda copy: copy.start())

    for buffer in (r_in, h_in):
        for share in range(SHARES):
            rows = slice(BLOCK * share + USED, BLOCK * (share + 1))
            buffer[rows, :] = jnp.zeros((BLOCK - USED, 128), f32)
    load_psi.wait()
    for i in range(THICK):
        for h in range(2):
            def put(a, value, i=i, h=h):
                psi_y[pl.ds(NG * i + 56 * h + a, 7, stride=8), :] = value

            to_rows(lambda b, i=i, h=h: psi[pl.ds(LINES * i + HALF * h + b, 7, stride=7), :], put)
    for k in range(THICK):
        kern[k] = kernel_tile(THICK * me + k, (128, 128))
    load_tab.wait()

    @pl.when(zh != 0)
    def _():
        pl.semaphore_wait(barrier, len(peers))

    def block(buffer, share, start, count):
        return buffer.at[pl.ds(BLOCK * share + start, count)]

    def exchange(source, target, send_sem, recv_sem, d, i, rows=ROWS):
        return send(
            block(source, share_of(d), ROWS * i, rows), block(target, me, ROWS * i, rows),
            send_sem, recv_sem, at_plane(d),
        )

    def keep(source, target):
        rows = pl.ds(pl.multiple_of(BLOCK * me, 8), BLOCK)
        target[rows, :] = source[rows, :]

    def of_all(i, row):
        return pl.ds(ROWS * i + row, SHARES, stride=BLOCK)

    def tucked(row, last, g):
        lanes = lax.broadcasted_iota(jnp.int32, row.shape, 1)
        return jnp.where(lanes < NG, row, pltpu.roll(last, NG - 16 * g, 1))

    def untucked(row):
        last = pltpu.roll(row(0), 16, 1)
        lanes = lax.broadcasted_iota(jnp.int32, last.shape, 1)
        for g in range(1, 7):
            last = jnp.where(lanes < 16 * g, last, pltpu.roll(row(g), 16 + 16 * g, 1))
        return last

    def forward(i):
        rows = slice(NG * i, NG * (i + 1))
        for j in range(2):
            for h in range(2):
                def put(a, value, j=j, h=h):
                    src_y[j, pl.ds(NG * i + 56 * h + a, 7, stride=8), :] = value

                to_rows(lambda b, j=j, h=h: src[j, h, i, pl.ds(b, 7, stride=7), :], put)
        field = psi_y[rows, :]
        density = jnp.concatenate([field * src_y[0, rows, :], field * src_y[1, rows, :]], axis=1)
        values = from_right(density, tab[0], tab[1])
        values = jnp.concatenate([values[:, 0:128], values[:, 128:256]], axis=0)
        values = from_left(tab[2, :, 0 : 2 * NG], tab[3, :, 0 : 2 * NG], values)
        for share in range(SHARES):
            start = BLOCK * share + ROWS * i
            s_out[start : start + ROWS, :] = values[16 * share : 16 * share + ROWS, :]

    def pass_on(i):
        @pl.when(zh != 0)
        def _():
            along_z(1, i).wait_recv()

        passed_on(i, lambda copy: copy.start())
        for d in (1, 3, 2):
            along_x(d, i).start()

    def take(i):
        gone = s_out.at[pl.ds(0, 3 * HALF)]
        send(gone, gone, xs.at[0, i], xr.at[i], at_x(1)).wait_recv()
        forward(i)
        for d in ORDER:
            exchange(s_out, r_in, fs, fr, d, i).start()

    def in_order(steps):
        for step in steps:
            (pass_on if step < 0 else take)(abs(step) - 1)

    @pl.when(zh == 2)
    def _():
        in_order(EVEN_FIRST)

    @pl.when(zh != 2)
    def _():
        in_order(ODD_FIRST)

    keep(s_out, r_in)
    whole = pl.ds(0, (SHARES - 1) * USED)
    packed = pl.ds(0, (SHARES - 1) * THICK * SENT)
    send(s_out.at[whole], r_in.at[whole], fs, fr, at_plane(1)).wait_recv()

    def first_part(waves):
        columns = []
        for k in waves:
            def row(t):
                return r_in[pl.ds(t, 128, stride=ROWS), :]

            columns.append(jnp.concatenate([row(k), row(THICK + k)], axis=0))
        spectrum = from_left(tab[4, 0 : 2 * NG], tab[5, 0 : 2 * NG], jnp.concatenate(columns, axis=1))
        factor = jnp.concatenate([kern[k, 0:NG] for k in waves], axis=1)
        return spectrum * jnp.concatenate([factor, factor], axis=0)

    def second_part(waves, spectrum, last):
        result = from_left(tab[6, :, 0 : 2 * NG], tab[7, :, 0 : 2 * NG], spectrum)
        if last is None:
            last = result[128:256]
        for place, k in enumerate(waves):
            lanes = slice(128 * place, 128 * (place + 1))
            g_out[pl.ds(k, 128, stride=ROWS), :] = tucked(result[0:128, lanes], last, k)
            g_out[pl.ds(THICK + k, 128, stride=ROWS), :] = result[128:256, lanes]
        return last

    groups = ((0, 1), (2, 3), (4, 5), (6,))
    held = [first_part(waves) for waves in groups]
    last = None
    for waves, spectrum in zip(groups[::-1], held[::-1]):
        last = second_part(waves, spectrum, last)

    for i in reversed(range(THICK)):
        for d in ORDER:
            exchange(g_out, h_in, bs, br.at[i], d, i, SENT).start()
    keep(g_out, h_in)

    def result(i):
        rows = pl.ds(LINES * i, LINES)
        return pltpu.make_async_copy(psi.at[rows], out.at[rows, 0], own_sem.at[i])

    out_lane = lax.broadcasted_iota(jnp.int32, (NG // 8, 128), 1)

    def back(i):
        h_in[of_all(i, SENT), :] = untucked(lambda g: h_in[of_all(i, g), :])
        columns = [h_in[BLOCK * q + ROWS * i : BLOCK * q + ROWS * i + 16, :] for q in range(SHARES)]
        values = from_left(tab[8, 0 : 2 * NG], tab[9, 0 : 2 * NG], jnp.concatenate(columns, axis=0))
        both = jnp.concatenate([values[0:NG], values[NG : 2 * NG]], axis=1)
        potential = from_right(both, tab[10], tab[11])
        rows = slice(NG * i, NG * (i + 1))
        psi_y[rows, :] = potential[:, 0:128] * src_y[0, rows, :] + potential[:, 128:256] * src_y[1, rows, :]
        turned = []
        for a in range(8):
            value = psi_y[pl.ds(NG * i + a, NG // 8, stride=8), :]
            turned.append(pltpu.roll(value, 128 - 16 * a, 1) if a else value)
        for b in range(7):
            value = jnp.where(out_lane < NG - 16 * b, turned[b], turned[b + 1])
            out[pl.ds(LINES * i + b, NG // 8, stride=7), 0, :] = value

    for i in reversed(range(THICK)):
        rows = pl.ds(0, (SHARES - 1) * SENT)
        send(g_out.at[rows], h_in.at[rows], bs, br.at[i], at_plane(1)).wait_recv()
        back(i)

    from_origin(lambda copy: copy.wait_send())
    for i in range(THICK):
        passed_on(i, lambda copy: copy.wait_send())
        for d in (1, 3, 2):
            along_x(d, i).wait_send()
    send(s_out.at[whole], r_in.at[whole], fs, fr, at_plane(1)).wait_send()
    send(g_out.at[packed], h_in.at[packed], bs, br.at[0], at_plane(1)).wait_send()


def on_device(orbitals):
    table = jnp.asarray(tables())
    field = orbitals.reshape(THICK * LINES, 1, 128)
    dma = pltpu.SemaphoreType.DMA
    vmem = pltpu.VMEM
    anywhere = pl.BlockSpec(memory_space=pl.ANY)
    half = pl.pallas_call(
        spread,
        out_shape=jax.ShapeDtypeStruct((THICK, 56, 128), f32),
        in_specs=[anywhere],
        out_specs=anywhere,
        scratch_shapes=[dma((THICK,)), dma((THICK,))],
        compiler_params=pltpu.CompilerParams(collective_id=1, has_side_effects=True),
    )(field)
    exchanged = vmem((SHARES * BLOCK, 128), f32)
    total = pl.pallas_call(
        body,
        out_shape=pltpu.VMEM((THICK * LINES, 1, 128), f32),
        in_specs=[anywhere] * 3,
        out_specs=pl.BlockSpec(memory_space=vmem),
        scratch_shapes=[
            vmem((THICK * LINES, 128), f32),
            vmem((12, 256, 256), bf16),
            vmem((2, 2, THICK, 56, 128), f32),
            vmem((THICK * NG, 128), f32),
            vmem((2, THICK * NG, 128), f32),
            vmem((THICK, 128, 128), f32),
            exchanged, exchanged, exchanged, exchanged,
            dma((2,)), dma((THICK,)), dma((3, THICK)), dma((THICK,)), dma((3, THICK)), dma((THICK,)),
            dma, dma, dma, dma((THICK,)),
        ],
        compiler_params=pltpu.CompilerParams(collective_id=0, has_side_effects=True),
    )(field, half, table)
    return total.reshape(orbitals.shape)


def solution(mesh):
    spec = P("band", "plane", None)
    return jax.shard_map(on_device, mesh=mesh, in_specs=(spec,), out_specs=spec, check_vma=False)
```

```python
import math

import jax
import jax.numpy as jnp
import ml_dtypes
import numpy as np
from jax import lax
from jax.experimental import pallas as pl
from jax.experimental.pallas import tpu as pltpu
from jax.sharding import PartitionSpec as P

MESH = pl.DeviceIdType.MESH
NG = 112
FLAT = NG * NG
LINES = FLAT // 128
HALF = LINES // 2
EVEN_FIRST = (-1, -3, -5, 1, 3, -2, 5, -4, -6, 2, -7, 4, 6, 7)
ODD_FIRST = (-2, -4, -6, -1, 2, -7, -3, 4, -5, 6, 1, 7, 3, 5)
SHARES = 16
THICK = NG // SHARES
ROWS = 2 * THICK
BLOCK = 112
SENT = ROWS - 1
USED = THICK * ROWS
ORDER = (10, 11, 8, 9, 6, 14, 7, 13, 2, 3, 4, 12, 5, 15, 1)
CROSSING_FIRST = (10, 11, 2, 3, 6, 14, 7, 15, 8, 9, 4, 12, 5, 13, 1)
screen_omega = 0.106
cell_length = 46.93
mixing = 0.25
f32, bf16 = jnp.float32, jnp.bfloat16


def tables():
    index = np.arange(NG)
    angle = (index[:, None] * index[None, :] % NG) * (2.0 * math.pi / NG)
    cos, sin = np.cos(angle), np.sin(angle)
    re, im = slice(0, NG), slice(128, 128 + NG)
    last = np.zeros((256, 256))
    last[re, re], last[im, re] = cos, sin
    last[re, im], last[im, im] = -sin, cos
    last_back = np.zeros((256, 256))
    last_back[re, re], last_back[im, re] = cos, -sin
    last_back[re, im], last_back[im, im] = sin, cos
    second = np.zeros((256, 256))
    second_back = np.zeros((256, 256))
    for share in range(SHARES):
        for part in range(2):
            for k in range(THICK):
                row, wave = 16 * share + THICK * part + k, THICK * share + k
                if part == 0:
                    second[row, 0:NG], second[row, NG : 2 * NG] = cos[wave], sin[wave]
                    second_back[0:NG, row], second_back[NG : 2 * NG, row] = cos[wave], sin[wave]
                else:
                    second[row, 0:NG], second[row, NG : 2 * NG] = -sin[wave], cos[wave]
                    second_back[0:NG, row], second_back[NG : 2 * NG, row] = -sin[wave], cos[wave]
    place = 8 * (index // THICK) + index % THICK
    first = np.zeros((256, 256))
    first_back = np.zeros((256, 256))
    first[re, place], first[re, 128 + place] = cos, sin
    tail = slice(NG, 2 * NG)
    first[tail, place], first[tail, 128 + place] = -sin, cos
    first_back[place, re], first_back[place, tail] = cos, -sin
    first_back[128 + place, re], first_back[128 + place, tail] = sin, cos
    both = []
    for table in (last, second, first, first_back, second_back, last_back):
        high = table.astype(ml_dtypes.bfloat16)
        both += [high, (table - high.astype(np.float64)).astype(ml_dtypes.bfloat16)]
    return np.stack(both)


def split(values):
    high = values.astype(bf16)
    return high, (values - high.astype(f32)).astype(bf16)


def dot(a, b):
    return jnp.dot(a, b, preferred_element_type=f32)


def from_left(high, low, values):
    big, small = split(values)
    return dot(high, big) + dot(high, small) + dot(low, big)


def from_right(values, high, low):
    big, small = split(values)
    return dot(big, high) + dot(small, high) + dot(big, low)


def kernel_tile(k_second, shape):
    def wave(index):
        return jnp.where(2 * index < NG, index, index - NG).astype(f32)

    first = wave(lax.broadcasted_iota(jnp.int32, shape, 0))
    last = wave(lax.broadcasted_iota(jnp.int32, shape, 1))
    second = wave(jnp.full(shape, k_second, jnp.int32))
    gsquare = (first * first + second * second + last * last) * (2.0 * math.pi / cell_length) ** 2
    safe = jnp.where(gsquare > 0, gsquare, 1.0)
    values = 4.0 * math.pi / safe * (1.0 - jnp.exp(-safe / (4.0 * screen_omega * screen_omega)))
    values = jnp.where(gsquare > 0, values, math.pi / (screen_omega * screen_omega))
    return values * (-mixing / float(NG) ** 3)


def kernel_axes():
    band = lax.axis_index("band")
    return band % 4, band // 4, lax.axis_index("plane")


def send(source, target, send_sem, recv_sem, device):
    return pltpu.make_async_remote_copy(
        src_ref=source, dst_ref=target, send_sem=send_sem, recv_sem=recv_sem,
        device_id=device, device_id_type=MESH,
    )


def spread(psi_hbm, half_hbm, send_sem, recv_sem):
    x, zh, me = kernel_axes()

    def half(i):
        return send(
            psi_hbm.at[pl.ds(LINES * i + HALF, HALF), 0], half_hbm.at[i, pl.ds(0, HALF)],
            send_sem.at[i], recv_sem.at[i], (zh * 4 + 3 - x, me),
        )

    @pl.when(zh == 0)
    def _():
        barrier = pltpu.get_barrier_semaphore()
        pl.semaphore_signal(barrier, inc=1, device_id=(zh * 4 + 3 - x, me), device_id_type=MESH)
        pl.semaphore_wait(barrier, 1)

        @pl.when(x < 2)
        def _():
            for i in range(THICK):
                half(i).start()
            for i in range(THICK):
                half(i).wait_send()

        @pl.when(x >= 2)
        def _():
            for i in range(THICK):
                half(i).wait_recv()


def body(
    psi_hbm, half_hbm, tab_hbm, out,
    psi, tab, src, psi_y, src_y, kern, s_out, r_in, g_out, h_in,
    load_sem, own_sem, zs, zr, xs, xr, fs, fr, bs, br,
):
    x, zh, me = kernel_axes()
    band = zh * 4 + x

    def at_x(d):
        return (zh * 4 + (x + d) % 4, me)

    def at_z(d):
        return (((zh + d) % 4) * 4 + x, me)

    def share_of(d):
        y, z, c = me // 4, (me // 2) % 2, me % 2
        return ((y + d // 4) % 4) * 4 + ((z + (d // 2) % 2) % 2) * 2 + (c + d % 2) % 2

    def at_plane(d):
        return (band, share_of(d))

    barrier = pltpu.get_barrier_semaphore()
    peers = [at_x(d) for d in (1, 2, 3)] + [at_z(d) for d in (1, 2, 3)]
    peers += [at_plane(d) for d in range(1, SHARES)]
    for peer in peers:
        pl.semaphore_signal(barrier, inc=1, device_id=peer, device_id_type=MESH)

    load_psi = pltpu.make_async_copy(psi_hbm.at[:, 0], psi, load_sem.at[0])
    load_psi.start()
    load_tab = pltpu.make_async_copy(tab_hbm, tab, load_sem.at[1])
    load_tab.start()

    own_source, own_half = ((x + 1) // 2) % 2, x // 2

    def piece(i):
        return src.at[own_source, own_half, i, pl.ds(0, HALF)]

    def own_from_psi(i):
        return pltpu.make_async_copy(psi_hbm.at[pl.ds(LINES * i, HALF), 0], piece(i), own_sem.at[i])

    def own_from_half(i):
        return pltpu.make_async_copy(half_hbm.at[i, pl.ds(0, HALF)], piece(i), own_sem.at[i])

    @pl.when(zh == 0)
    def _():
        @pl.when(x < 2)
        def _():
            for i in range(THICK):
                own_from_psi(i).start()

        @pl.when(x >= 2)
        def _():
            for i in range(THICK):
                own_from_half(i).start()

    lane = lax.broadcasted_iota(jnp.int32, (HALF // 7, 128), 1)

    def to_rows(rows, at):
        flat = [rows(b) for b in range(7)]
        for a in range(8):
            if a == 0:
                value = flat[0]
            else:
                below = flat[a] if a < 7 else jnp.zeros_like(flat[0])
                value = pltpu.roll(jnp.where(lane < 128 - 16 * a, below, flat[a - 1]), 16 * a, 1)
            at(a, value)

    def along_z(d, i):
        return send(piece(i), piece(i), zs.at[d - 1, i], zr.at[i], at_z(d))

    def along_x(d, i):
        return send(piece(i), piece(i), xs.at[d - 1, i], xr.at[i], at_x(d))

    def from_origin(act):
        @pl.when(zh == 0)
        def _():
            for i in (0, 2, 4):
                act(along_z(2, i))
            for i in (1, 3, 5, 6):
                for d in (3, 1):
                    act(along_z(d, i))

    def passed_on(i, act):
        relay = (2, 1, 2, 3, 2, 1, 3)[i]

        @pl.when(zh == relay)
        def _():
            for d in (1, 3) if relay == 2 else (relay,):
                act(along_z(d, i))

    @pl.when(zh == 0)
    def _():
        for i in range(THICK):
            own_from_psi(i).wait()
        pl.semaphore_wait(barrier, len(peers))

    from_origin(lambda copy: copy.start())

    for buffer in (r_in, h_in):
        for share in range(SHARES):
            rows = slice(BLOCK * share + USED, BLOCK * (share + 1))
            buffer[rows, :] = jnp.zeros((BLOCK - USED, 128), f32)
    load_psi.wait()
    for i in range(THICK):
        for h in range(2):
            def put(a, value, i=i, h=h):
                psi_y[pl.ds(NG * i + 56 * h + a, 7, stride=8), :] = value

            to_rows(lambda b, i=i, h=h: psi[pl.ds(LINES * i + HALF * h + b, 7, stride=7), :], put)
    for k in range(THICK):
        kern[k] = kernel_tile(THICK * me + k, (128, 128))
    load_tab.wait()

    @pl.when(zh != 0)
    def _():
        pl.semaphore_wait(barrier, len(peers))

    def block(buffer, share, start, count):
        return buffer.at[pl.ds(BLOCK * share + start, count)]

    def exchange(source, target, send_sem, recv_sem, d, i, rows=ROWS):
        return send(
            block(source, share_of(d), ROWS * i, rows), block(target, me, ROWS * i, rows),
            send_sem, recv_sem, at_plane(d),
        )

    def keep(source, target):
        rows = pl.ds(pl.multiple_of(BLOCK * me, 8), BLOCK)
        target[rows, :] = source[rows, :]

    def of_all(i, row):
        return pl.ds(ROWS * i + row, SHARES, stride=BLOCK)

    def tucked(row, last, g):
        lanes = lax.broadcasted_iota(jnp.int32, row.shape, 1)
        return jnp.where(lanes < NG, row, pltpu.roll(last, NG - 16 * g, 1))

    def untucked(row):
        last = pltpu.roll(row(0), 16, 1)
        lanes = lax.broadcasted_iota(jnp.int32, last.shape, 1)
        for g in range(1, 7):
            last = jnp.where(lanes < 16 * g, last, pltpu.roll(row(g), 16 + 16 * g, 1))
        return last

    def forward(i):
        rows = slice(NG * i, NG * (i + 1))
        for j in range(2):
            for h in range(2):
                def put(a, value, j=j, h=h):
                    src_y[j, pl.ds(NG * i + 56 * h + a, 7, stride=8), :] = value

                to_rows(lambda b, j=j, h=h: src[j, h, i, pl.ds(b, 7, stride=7), :], put)
        field = psi_y[rows, :]
        density = jnp.concatenate([field * src_y[0, rows, :], field * src_y[1, rows, :]], axis=1)
        values = from_right(density, tab[0], tab[1])
        values = jnp.concatenate([values[:, 0:128], values[:, 128:256]], axis=0)
        values = from_left(tab[2, :, 0 : 2 * NG], tab[3, :, 0 : 2 * NG], values)
        for share in range(SHARES):
            start = BLOCK * share + ROWS * i
            s_out[start : start + ROWS, :] = values[16 * share : 16 * share + ROWS, :]

    def pass_on(i):
        @pl.when(zh != 0)
        def _():
            along_z(1, i).wait_recv()

        passed_on(i, lambda copy: copy.start())
        for d in (1, 3, 2):
            along_x(d, i).start()

    def take(i):
        gone = s_out.at[pl.ds(0, 3 * HALF)]
        send(gone, gone, xs.at[0, i], xr.at[i], at_x(1)).wait_recv()
        forward(i)
        for d in CROSSING_FIRST:
            exchange(s_out, r_in, fs, fr, d, i).start()

    def in_order(steps):
        for step in steps:
            (pass_on if step < 0 else take)(abs(step) - 1)

    @pl.when(zh == 2)
    def _():
        in_order(EVEN_FIRST)

    @pl.when(zh != 2)
    def _():
        in_order(ODD_FIRST)

    keep(s_out, r_in)
    whole = pl.ds(0, (SHARES - 1) * USED)
    packed = pl.ds(0, (SHARES - 1) * THICK * SENT)
    send(s_out.at[whole], r_in.at[whole], fs, fr, at_plane(1)).wait_recv()

    def first_part(waves):
        columns = []
        for k in waves:
            def row(t):
                return r_in[pl.ds(t, 128, stride=ROWS), :]

            columns.append(jnp.concatenate([row(k), row(THICK + k)], axis=0))
        spectrum = from_left(tab[4, 0 : 2 * NG], tab[5, 0 : 2 * NG], jnp.concatenate(columns, axis=1))
        factor = jnp.concatenate([kern[k, 0:NG] for k in waves], axis=1)
        return spectrum * jnp.concatenate([factor, factor], axis=0)

    def second_part(waves, spectrum, last):
        result = from_left(tab[6, :, 0 : 2 * NG], tab[7, :, 0 : 2 * NG], spectrum)
        if last is None:
            last = result[128:256]
        for place, k in enumerate(waves):
            lanes = slice(128 * place, 128 * (place + 1))
            g_out[pl.ds(k, 128, stride=ROWS), :] = tucked(result[0:128, lanes], last, k)
            g_out[pl.ds(THICK + k, 128, stride=ROWS), :] = result[128:256, lanes]
        return last

    groups = ((0, 1), (2, 3), (4, 5), (6,))
    held = [first_part(waves) for waves in groups]
    last = None
    for waves, spectrum in zip(groups[::-1], held[::-1]):
        last = second_part(waves, spectrum, last)

    for i in reversed(range(THICK)):
        for d in ORDER:
            exchange(g_out, h_in, bs, br.at[i], d, i, SENT).start()
    keep(g_out, h_in)

    def result(i):
        rows = pl.ds(LINES * i, LINES)
        return pltpu.make_async_copy(psi.at[rows], out.at[rows, 0], own_sem.at[i])

    out_lane = lax.broadcasted_iota(jnp.int32, (NG // 8, 128), 1)

    def back(i):
        h_in[of_all(i, SENT), :] = untucked(lambda g: h_in[of_all(i, g), :])
        columns = [h_in[BLOCK * q + ROWS * i : BLOCK * q + ROWS * i + 16, :] for q in range(SHARES)]
        values = from_left(tab[8, 0 : 2 * NG], tab[9, 0 : 2 * NG], jnp.concatenate(columns, axis=0))
        both = jnp.concatenate([values[0:NG], values[NG : 2 * NG]], axis=1)
        potential = from_right(both, tab[10], tab[11])
        rows = slice(NG * i, NG * (i + 1))
        psi_y[rows, :] = potential[:, 0:128] * src_y[0, rows, :] + potential[:, 128:256] * src_y[1, rows, :]
        turned = []
        for a in range(8):
            value = psi_y[pl.ds(NG * i + a, NG // 8, stride=8), :]
            turned.append(pltpu.roll(value, 128 - 16 * a, 1) if a else value)
        for b in range(7):
            value = jnp.where(out_lane < NG - 16 * b, turned[b], turned[b + 1])
            out[pl.ds(LINES * i + b, NG // 8, stride=7), 0, :] = value

    for i in reversed(range(THICK)):
        rows = pl.ds(0, (SHARES - 1) * SENT)
        send(g_out.at[rows], h_in.at[rows], bs, br.at[i], at_plane(1)).wait_recv()
        back(i)

    from_origin(lambda copy: copy.wait_send())
    for i in range(THICK):
        passed_on(i, lambda copy: copy.wait_send())
        for d in (1, 3, 2):
            along_x(d, i).wait_send()
    send(s_out.at[whole], r_in.at[whole], fs, fr, at_plane(1)).wait_send()
    send(g_out.at[packed], h_in.at[packed], bs, br.at[0], at_plane(1)).wait_send()


def on_device(orbitals):
    table = jnp.asarray(tables())
    field = orbitals.reshape(THICK * LINES, 1, 128)
    dma = pltpu.SemaphoreType.DMA
    vmem = pltpu.VMEM
    anywhere = pl.BlockSpec(memory_space=pl.ANY)
    half = pl.pallas_call(
        spread,
        out_shape=jax.ShapeDtypeStruct((THICK, 56, 128), f32),
        in_specs=[anywhere],
        out_specs=anywhere,
        scratch_shapes=[dma((THICK,)), dma((THICK,))],
        compiler_params=pltpu.CompilerParams(collective_id=1, has_side_effects=True),
    )(field)
    exchanged = vmem((SHARES * BLOCK, 128), f32)
    total = pl.pallas_call(
        body,
        out_shape=pltpu.VMEM((THICK * LINES, 1, 128), f32),
        in_specs=[anywhere] * 3,
        out_specs=pl.BlockSpec(memory_space=vmem),
        scratch_shapes=[
            vmem((THICK * LINES, 128), f32),
            vmem((12, 256, 256), bf16),
            vmem((2, 2, THICK, 56, 128), f32),
            vmem((THICK * NG, 128), f32),
            vmem((2, THICK * NG, 128), f32),
            vmem((THICK, 128, 128), f32),
            exchanged, exchanged, exchanged, exchanged,
            dma((2,)), dma((THICK,)), dma((3, THICK)), dma((THICK,)), dma((3, THICK)), dma((THICK,)),
            dma, dma, dma, dma((THICK,)),
        ],
        compiler_params=pltpu.CompilerParams(collective_id=0, has_side_effects=True),
    )(field, half, table)
    return total.reshape(orbitals.shape)


def solution(mesh):
    spec = P("band", "plane", None)
    return jax.shard_map(on_device, mesh=mesh, in_specs=(spec,), out_specs=spec, check_vma=False)
```

```python
import math

import jax
import jax.numpy as jnp
import ml_dtypes
import numpy as np
from jax import lax
from jax.experimental import pallas as pl
from jax.experimental.pallas import tpu as pltpu
from jax.sharding import PartitionSpec as P

MESH = pl.DeviceIdType.MESH
NG = 112
FLAT = NG * NG
LINES = FLAT // 128
HALF = LINES // 2
EVEN_FIRST = (-1, -3, -5, 1, 3, -2, 5, -4, -6, 2, -7, 4, 6, 7)
ODD_FIRST = (-2, -4, -6, -1, 2, -7, -3, 4, -5, 6, 1, 7, 3, 5)
SHARES = 16
THICK = NG // SHARES
ROWS = 2 * THICK
BLOCK = 112
SENT = ROWS - 1
USED = THICK * ROWS
ORDER = (10, 11, 8, 9, 6, 14, 7, 13, 2, 3, 4, 12, 5, 15, 1)
screen_omega = 0.106
cell_length = 46.93
mixing = 0.25
f32, bf16 = jnp.float32, jnp.bfloat16


def tables():
    index = np.arange(NG)
    angle = (index[:, None] * index[None, :] % NG) * (2.0 * math.pi / NG)
    cos, sin = np.cos(angle), np.sin(angle)
    re, im = slice(0, NG), slice(128, 128 + NG)
    last = np.zeros((256, 256))
    last[re, re], last[im, re] = cos, sin
    last[re, im], last[im, im] = -sin, cos
    last_back = np.zeros((256, 256))
    last_back[re, re], last_back[im, re] = cos, -sin
    last_back[re, im], last_back[im, im] = sin, cos
    second = np.zeros((256, 256))
    second_back = np.zeros((256, 256))
    for share in range(SHARES):
        for part in range(2):
            for k in range(THICK):
                row, wave = 16 * share + THICK * part + k, THICK * share + k
                if part == 0:
                    second[row, 0:NG], second[row, NG : 2 * NG] = cos[wave], sin[wave]
                    second_back[0:NG, row], second_back[NG : 2 * NG, row] = cos[wave], sin[wave]
                else:
                    second[row, 0:NG], second[row, NG : 2 * NG] = -sin[wave], cos[wave]
                    second_back[0:NG, row], second_back[NG : 2 * NG, row] = -sin[wave], cos[wave]
    place = 8 * (index // THICK) + index % THICK
    first = np.zeros((256, 256))
    first_back = np.zeros((256, 256))
    first[re, place], first[re, 128 + place] = cos, sin
    tail = slice(NG, 2 * NG)
    first[tail, place], first[tail, 128 + place] = -sin, cos
    first_back[place, re], first_back[place, tail] = cos, -sin
    first_back[128 + place, re], first_back[128 + place, tail] = sin, cos
    both = []
    for table in (last, second, first, first_back, second_back, last_back):
        high = table.astype(ml_dtypes.bfloat16)
        both += [high, (table - high.astype(np.float64)).astype(ml_dtypes.bfloat16)]
    return np.stack(both)


def split(values):
    high = values.astype(bf16)
    return high, (values - high.astype(f32)).astype(bf16)


def dot(a, b):
    return jnp.dot(a, b, preferred_element_type=f32)


def from_left(high, low, values):
    big, small = split(values)
    return dot(high, big) + dot(high, small) + dot(low, big)


def from_right(values, high, low):
    big, small = split(values)
    return dot(big, high) + dot(small, high) + dot(big, low)


def kernel_tile(k_second, shape):
    def wave(index):
        return jnp.where(2 * index < NG, index, index - NG).astype(f32)

    first = wave(lax.broadcasted_iota(jnp.int32, shape, 0))
    last = wave(lax.broadcasted_iota(jnp.int32, shape, 1))
    second = wave(jnp.full(shape, k_second, jnp.int32))
    gsquare = (first * first + second * second + last * last) * (2.0 * math.pi / cell_length) ** 2
    safe = jnp.where(gsquare > 0, gsquare, 1.0)
    values = 4.0 * math.pi / safe * (1.0 - jnp.exp(-safe / (4.0 * screen_omega * screen_omega)))
    values = jnp.where(gsquare > 0, values, math.pi / (screen_omega * screen_omega))
    return values * (-mixing / float(NG) ** 3)


def kernel_axes():
    band = lax.axis_index("band")
    return band % 4, band // 4, lax.axis_index("plane")


def send(source, target, send_sem, recv_sem, device):
    return pltpu.make_async_remote_copy(
        src_ref=source, dst_ref=target, send_sem=send_sem, recv_sem=recv_sem,
        device_id=device, device_id_type=MESH,
    )


def spread(psi_hbm, half_hbm, send_sem, recv_sem):
    x, zh, me = kernel_axes()

    def half(i):
        return send(
            psi_hbm.at[pl.ds(LINES * i + HALF, HALF), 0], half_hbm.at[i, pl.ds(0, HALF)],
            send_sem.at[i], recv_sem.at[i], (zh * 4 + 3 - x, me),
        )

    @pl.when(zh == 0)
    def _():
        barrier = pltpu.get_barrier_semaphore()
        pl.semaphore_signal(barrier, inc=1, device_id=(zh * 4 + 3 - x, me), device_id_type=MESH)
        pl.semaphore_wait(barrier, 1)

        @pl.when(x < 2)
        def _():
            for i in range(THICK):
                half(i).start()
            for i in range(THICK):
                half(i).wait_send()

        @pl.when(x >= 2)
        def _():
            for i in range(THICK):
                half(i).wait_recv()


def body(
    psi_hbm, half_hbm, tab_hbm, out,
    psi, tab, src, psi_y, src_y, kern, s_out, r_in, g_out, h_in,
    load_sem, own_sem, zs, zr, xs, xr, fs, fr, bs, br,
):
    x, zh, me = kernel_axes()
    band = zh * 4 + x

    def at_x(d):
        return (zh * 4 + (x + d) % 4, me)

    def at_z(d):
        return (((zh + d) % 4) * 4 + x, me)

    def share_of(d):
        y, z, c = me // 4, (me // 2) % 2, me % 2
        return ((y + d // 4) % 4) * 4 + ((z + (d // 2) % 2) % 2) * 2 + (c + d % 2) % 2

    def at_plane(d):
        return (band, share_of(d))

    barrier = pltpu.get_barrier_semaphore()
    peers = [at_x(d) for d in (1, 2, 3)] + [at_z(d) for d in (1, 2, 3)]
    peers += [at_plane(d) for d in range(1, SHARES)]
    for peer in peers:
        pl.semaphore_signal(barrier, inc=1, device_id=peer, device_id_type=MESH)

    load_psi = pltpu.make_async_copy(psi_hbm.at[:, 0], psi, load_sem.at[0])
    load_psi.start()
    load_tab = pltpu.make_async_copy(tab_hbm, tab, load_sem.at[1])
    load_tab.start()

    own_source, own_half = ((x + 1) // 2) % 2, x // 2

    def piece(i):
        return src.at[own_source, own_half, i, pl.ds(0, HALF)]

    def own_from_psi(i):
        return pltpu.make_async_copy(psi_hbm.at[pl.ds(LINES * i, HALF), 0], piece(i), own_sem.at[i])

    def own_from_half(i):
        return pltpu.make_async_copy(half_hbm.at[i, pl.ds(0, HALF)], piece(i), own_sem.at[i])

    @pl.when(zh == 0)
    def _():
        @pl.when(x < 2)
        def _():
            for i in range(THICK):
                own_from_psi(i).start()

        @pl.when(x >= 2)
        def _():
            for i in range(THICK):
                own_from_half(i).start()

    lane = lax.broadcasted_iota(jnp.int32, (HALF // 7, 128), 1)

    def to_rows(rows, at):
        flat = [rows(b) for b in range(7)]
        for a in range(8):
            if a == 0:
                value = flat[0]
            else:
                below = flat[a] if a < 7 else jnp.zeros_like(flat[0])
                value = pltpu.roll(jnp.where(lane < 128 - 16 * a, below, flat[a - 1]), 16 * a, 1)
            at(a, value)

    def along_z(d, i):
        return send(piece(i), piece(i), zs.at[d - 1, i], zr.at[i], at_z(d))

    def along_x(d, i):
        return send(piece(i), piece(i), xs.at[d - 1, i], xr.at[i], at_x(d))

    def from_origin(act):
        @pl.when(zh == 0)
        def _():
            for i in (0, 2, 4):
                act(along_z(2, i))
            for i in (1, 3, 5, 6):
                for d in (3, 1):
                    act(along_z(d, i))

    def passed_on(i, act):
        relay = (2, 1, 2, 3, 2, 1, 3)[i]

        @pl.when(zh == relay)
        def _():
            for d in (1, 3) if relay == 2 else (relay,):
                act(along_z(d, i))

    @pl.when(zh == 0)
    def _():
        for i in range(THICK):
            own_from_psi(i).wait()
        pl.semaphore_wait(barrier, len(peers))

    from_origin(lambda copy: copy.start())

    for buffer in (r_in, h_in):
        for share in range(SHARES):
            rows = slice(BLOCK * share + USED, BLOCK * (share + 1))
            buffer[rows, :] = jnp.zeros((BLOCK - USED, 128), f32)
    load_psi.wait()
    for i in range(THICK):
        for h in range(2):
            def put(a, value, i=i, h=h):
                psi_y[pl.ds(NG * i + 56 * h + a, 7, stride=8), :] = value

            to_rows(lambda b, i=i, h=h: psi[pl.ds(LINES * i + HALF * h + b, 7, stride=7), :], put)
    for k in range(THICK):
        kern[k] = kernel_tile(THICK * me + k, (128, 128))
    load_tab.wait()

    @pl.when(zh != 0)
    def _():
        pl.semaphore_wait(barrier, len(peers))

    def block(buffer, share, start, count):
        return buffer.at[pl.ds(BLOCK * share + start, count)]

    def exchange(source, target, send_sem, recv_sem, d, i, rows=ROWS):
        return send(
            block(source, share_of(d), ROWS * i, rows), block(target, me, ROWS * i, rows),
            send_sem, recv_sem, at_plane(d),
        )

    def keep(source, target):
        rows = pl.ds(pl.multiple_of(BLOCK * me, 8), BLOCK)
        target[rows, :] = source[rows, :]

    def of_all(i, row):
        return pl.ds(ROWS * i + row, SHARES, stride=BLOCK)

    def tucked(row, last, g):
        lanes = lax.broadcasted_iota(jnp.int32, row.shape, 1)
        return jnp.where(lanes < NG, row, pltpu.roll(last, NG - 16 * g, 1))

    def untucked(row):
        last = pltpu.roll(row(0), 16, 1)
        lanes = lax.broadcasted_iota(jnp.int32, last.shape, 1)
        for g in range(1, 7):
            last = jnp.where(lanes < 16 * g, last, pltpu.roll(row(g), 16 + 16 * g, 1))
        return last

    def forward(i):
        rows = slice(NG * i, NG * (i + 1))
        for j in range(2):
            for h in range(2):
                def put(a, value, j=j, h=h):
                    src_y[j, pl.ds(NG * i + 56 * h + a, 7, stride=8), :] = value

                to_rows(lambda b, j=j, h=h: src[j, h, i, pl.ds(b, 7, stride=7), :], put)
        field = psi_y[rows, :]
        density = jnp.concatenate([field * src_y[0, rows, :], field * src_y[1, rows, :]], axis=1)
        values = from_right(density, tab[0], tab[1])
        values = jnp.concatenate([values[:, 0:128], values[:, 128:256]], axis=0)
        values = from_left(tab[2, :, 0 : 2 * NG], tab[3, :, 0 : 2 * NG], values)
        for share in range(SHARES):
            start = BLOCK * share + ROWS * i
            s_out[start : start + ROWS, :] = values[16 * share : 16 * share + ROWS, :]

    def pass_on(i):
        @pl.when(zh != 0)
        def _():
            along_z(1, i).wait_recv()

        passed_on(i, lambda copy: copy.start())
        for d in (2, 1, 3):
            along_x(d, i).start()

    def take(i):
        gone = s_out.at[pl.ds(0, 3 * HALF)]
        send(gone, gone, xs.at[0, i], xr.at[i], at_x(1)).wait_recv()
        forward(i)
        for d in ORDER:
            exchange(s_out, r_in, fs, fr, d, i).start()

    def in_order(steps):
        for step in steps:
            (pass_on if step < 0 else take)(abs(step) - 1)

    @pl.when(zh == 2)
    def _():
        in_order(EVEN_FIRST)

    @pl.when(zh != 2)
    def _():
        in_order(ODD_FIRST)

    keep(s_out, r_in)
    whole = pl.ds(0, (SHARES - 1) * USED)
    packed = pl.ds(0, (SHARES - 1) * THICK * SENT)
    send(s_out.at[whole], r_in.at[whole], fs, fr, at_plane(1)).wait_recv()

    def first_part(waves):
        columns = []
        for k in waves:
            def row(t):
                return r_in[pl.ds(t, 128, stride=ROWS), :]

            columns.append(jnp.concatenate([row(k), row(THICK + k)], axis=0))
        spectrum = from_left(tab[4, 0 : 2 * NG], tab[5, 0 : 2 * NG], jnp.concatenate(columns, axis=1))
        factor = jnp.concatenate([kern[k, 0:NG] for k in waves], axis=1)
        return spectrum * jnp.concatenate([factor, factor], axis=0)

    def second_part(waves, spectrum, last):
        result = from_left(tab[6, :, 0 : 2 * NG], tab[7, :, 0 : 2 * NG], spectrum)
        if last is None:
            last = result[128:256]
        for place, k in enumerate(waves):
            lanes = slice(128 * place, 128 * (place + 1))
            g_out[pl.ds(k, 128, stride=ROWS), :] = tucked(result[0:128, lanes], last, k)
            g_out[pl.ds(THICK + k, 128, stride=ROWS), :] = result[128:256, lanes]
        return last

    groups = ((0, 1), (2, 3), (4, 5), (6,))
    held = [first_part(waves) for waves in groups]
    last = None
    for waves, spectrum in zip(groups[::-1], held[::-1]):
        last = second_part(waves, spectrum, last)

    for i in reversed(range(THICK)):
        for d in ORDER:
            exchange(g_out, h_in, bs, br.at[i], d, i, SENT).start()
    keep(g_out, h_in)

    def result(i):
        rows = pl.ds(LINES * i, LINES)
        return pltpu.make_async_copy(psi.at[rows], out.at[rows, 0], own_sem.at[i])

    out_lane = lax.broadcasted_iota(jnp.int32, (NG // 8, 128), 1)

    def back(i):
        h_in[of_all(i, SENT), :] = untucked(lambda g: h_in[of_all(i, g), :])
        columns = [h_in[BLOCK * q + ROWS * i : BLOCK * q + ROWS * i + 16, :] for q in range(SHARES)]
        values = from_left(tab[8, 0 : 2 * NG], tab[9, 0 : 2 * NG], jnp.concatenate(columns, axis=0))
        both = jnp.concatenate([values[0:NG], values[NG : 2 * NG]], axis=1)
        potential = from_right(both, tab[10], tab[11])
        rows = slice(NG * i, NG * (i + 1))
        psi_y[rows, :] = potential[:, 0:128] * src_y[0, rows, :] + potential[:, 128:256] * src_y[1, rows, :]
        turned = []
        for a in range(8):
            value = psi_y[pl.ds(NG * i + a, NG // 8, stride=8), :]
            turned.append(pltpu.roll(value, 128 - 16 * a, 1) if a else value)
        for b in range(7):
            value = jnp.where(out_lane < NG - 16 * b, turned[b], turned[b + 1])
            out[pl.ds(LINES * i + b, NG // 8, stride=7), 0, :] = value

    for i in reversed(range(THICK)):
        rows = pl.ds(0, (SHARES - 1) * SENT)
        send(g_out.at[rows], h_in.at[rows], bs, br.at[i], at_plane(1)).wait_recv()
        back(i)

    from_origin(lambda copy: copy.wait_send())
    for i in range(THICK):
        passed_on(i, lambda copy: copy.wait_send())
        for d in (2, 1, 3):
            along_x(d, i).wait_send()
    send(s_out.at[whole], r_in.at[whole], fs, fr, at_plane(1)).wait_send()
    send(g_out.at[packed], h_in.at[packed], bs, br.at[0], at_plane(1)).wait_send()


def on_device(orbitals):
    table = jnp.asarray(tables())
    field = orbitals.reshape(THICK * LINES, 1, 128)
    dma = pltpu.SemaphoreType.DMA
    vmem = pltpu.VMEM
    anywhere = pl.BlockSpec(memory_space=pl.ANY)
    half = pl.pallas_call(
        spread,
        out_shape=jax.ShapeDtypeStruct((THICK, 56, 128), f32),
        in_specs=[anywhere],
        out_specs=anywhere,
        scratch_shapes=[dma((THICK,)), dma((THICK,))],
        compiler_params=pltpu.CompilerParams(collective_id=1, has_side_effects=True),
    )(field)
    exchanged = vmem((SHARES * BLOCK, 128), f32)
    total = pl.pallas_call(
        body,
        out_shape=pltpu.VMEM((THICK * LINES, 1, 128), f32),
        in_specs=[anywhere] * 3,
        out_specs=pl.BlockSpec(memory_space=vmem),
        scratch_shapes=[
            vmem((THICK * LINES, 128), f32),
            vmem((12, 256, 256), bf16),
            vmem((2, 2, THICK, 56, 128), f32),
            vmem((THICK * NG, 128), f32),
            vmem((2, THICK * NG, 128), f32),
            vmem((THICK, 128, 128), f32),
            exchanged, exchanged, exchanged, exchanged,
            dma((2,)), dma((THICK,)), dma((3, THICK)), dma((THICK,)), dma((3, THICK)), dma((THICK,)),
            dma, dma, dma, dma((THICK,)),
        ],
        compiler_params=pltpu.CompilerParams(collective_id=0, has_side_effects=True),
    )(field, half, table)
    return total.reshape(orbitals.shape)


def solution(mesh):
    spec = P("band", "plane", None)
    return jax.shard_map(on_device, mesh=mesh, in_specs=(spec,), out_specs=spec, check_vma=False)
```
